256 devices in a mesh: wide: 16 (over z_hi, x), narrow: 4 (over y), depth: 4 (over z_lo, core).
Axes of the slice: x: 4, y: 4, z: 8 (z_hi: 4, z_lo: 2; z = z_hi * 2 + z_lo), core: 2. Of those that a mesh axis runs over, the one named last changes fastest.
Arguments:
- patch_store: bfloat16 [64, 1024, 4096], P('wide', 'depth'), may hold values from -6 to 6
- w_key: bfloat16 [4096, 1024], P(None, 'narrow'), may hold values from -0.09375 to 0.09375
- w_value: bfloat16 [4096, 1024], P(None, 'narrow'), may hold values from -0.09375 to 0.09375
- key_gain: float32 [128], replicated, may hold values from 0.1 to 1.9
- query_gain: float32 [128], replicated, may hold values from 0.1 to 1.9
- queries: bfloat16 [256, 4096], P('wide', 'narrow'), may hold values from -6 to 6
- owner_table: int32 [64], replicated, may hold values from 0 to 63, each once
- reader_table: int32 [16, 2], replicated, may hold values from 0 to 63
- request_image: int32 [256], P('wide'), may hold values from 0 to 1
- image_tiles: int32 [64], replicated, may hold values from 1 to 4
Outputs:
- context: bfloat16 [256, 4096], P(('wide', 'depth'), 'narrow')
The draws below stay inside these ranges and needn't reach their ends.
Inputs may be any that keep to these rules, and one draw needn't show every extreme that they name: owner_table is a permutation of the slots. `reader_table`: entries are image ids; a group's list may repeat an image.
All inputs are finite; a program needn't handle non-finite values.
Results may differ from the reference program's by a relative error of at most 0.012.
Values may be sent and summed in bfloat16 or wider, within the bound.
A program may use at most 64 MiB of HBM per device.

```python
import math
import jax
import jax.numpy as jnp
import numpy as np
from jax import lax

D = 4096
HEADS = 32
KV_HEADS = 8
HD = 128
TILES = 4
TILE_P = 256
READS = 2
PATCHES = 1024
IMAGES = 64
GROUPS = 16
BATCH = 256
N_WIDE = 16


def touch_ends(values, own_key, smallest, largest):
    place = [jax.random.randint(jax.random.fold_in(own_key, axis), (), 0, length) for axis, length in enumerate(values.shape)]
    main_axis = values.shape.index(max(values.shape))
    neighbour = place[:main_axis] + [(place[main_axis] + 1) % values.shape[main_axis]] + place[main_axis + 1:]
    return values.at[tuple(place)].set(smallest).at[tuple(neighbour)].set(largest)


def shard_levels(own_key, extent, split, smallest, high):
    def one(position, parts):
        heights = jax.random.uniform(jax.random.fold_in(jax.random.fold_in(own_key, 6), position), (parts,), jnp.float32, smallest / len(split), high / len(split))
        return jnp.repeat(jnp.exp(heights), extent[position] // parts).reshape((-1,) + (1,) * (len(extent) - position - 1))

    factor_of = one(*split[0])
    for cut in split[1:]:
        factor_of = factor_of * one(*cut)
    return factor_of


def rank_table(count, slope):
    portions = [(1 << 20) // math.isqrt(rank ** slope) + 1 for rank in range(1, count + 1)]
    spread = 1 + sum(portions) // (1 << 30)
    return np.cumsum(np.array([max(1, weight // spread) for weight in portions]))


def ranked_ids(key, extent, number_of, skew):
    table = rank_table(number_of, skew)
    lot = jax.random.randint(jax.random.fold_in(key, 1), extent, 0, int(table[number_of - 1]))
    standing = jnp.searchsorted(jnp.asarray(table, jnp.int32), lot, side="right")
    return jax.random.permutation(jax.random.fold_in(key, 2), number_of)[standing].astype(jnp.int32)


def centred(stream_key, shape, spread, reach, split=(), held_as=jnp.bfloat16):
    factor_of = shard_levels(stream_key, shape, split, -0.22, 0.18) if split else 1.0
    drawn = jax.random.normal(stream_key, shape, jnp.float32) * spread * factor_of
    return jnp.minimum(jnp.maximum(drawn, -reach), reach).astype(held_as)


def setup_inputs(seed: int = 0) -> dict:
    streams_of = jax.random.split(jax.random.key(seed), 11)
    return {
        "patch_store": centred(streams_of[0], (IMAGES, PATCHES, D), 1.0, 6.0, ((0, 16), (1, 4))),
        "w_key": centred(streams_of[1], (D, KV_HEADS * HD), D ** -0.5, 0.09375, ((1, 4),)),
        "w_value": centred(streams_of[2], (D, KV_HEADS * HD), D ** -0.5, 0.09375, ((1, 4),)),
        "key_gain": jnp.clip(1.0 + 0.18 * jax.random.normal(streams_of[3], (HD,), jnp.float32), 0.1, 1.9),
        "query_gain": jnp.clip(1.0 + 0.18 * jax.random.normal(streams_of[4], (HD,), jnp.float32), 0.1, 1.9),
        "queries": centred(streams_of[5], (BATCH, HEADS * HD), 1.0, 6.0, ((0, 16), (1, 4))),
        "owner_table": jax.random.permutation(streams_of[6], IMAGES).astype(jnp.int32),
        "reader_table": touch_ends(ranked_ids(streams_of[7], (GROUPS, READS), IMAGES, 1), jax.random.fold_in(streams_of[7], 3), 0, IMAGES - 1).astype(jnp.int32),
        "request_image": touch_ends(jax.random.randint(streams_of[8], (BATCH,), 0, READS), jax.random.fold_in(streams_of[8], 1), 0, READS - 1).astype(jnp.int32),
        "image_tiles": touch_ends(jax.random.randint(streams_of[9], (IMAGES,), 1, TILES + 1), jax.random.fold_in(streams_of[9], 1), 1, TILES).astype(jnp.int32),
    }


epsilon = 1e-05

def rms_scaled(tensor, scaling):
    return tensor / jnp.sqrt(lax.optimization_barrier(jnp.mean(tensor * tensor, axis=-1, keepdims=True)) + epsilon) * scaling

def reference(patch_store, w_key, w_value, key_gain, query_gain, queries, owner_table, reader_table, request_image, image_tiles):
    batch = queries.shape[0]
    per_group = batch // N_WIDE
    group_size = HEADS // KV_HEADS
    scale = 1.0 / math.sqrt(HD)

    def one_group(group_index):
        images = reader_table[group_index]
        slots = owner_table[images]
        patch_rows = patch_store[slots].reshape(READS * PATCHES, D)
        raw_keys = jnp.dot(patch_rows, w_key, preferred_element_type=jnp.float32).reshape(READS, PATCHES, KV_HEADS, HD)
        image_keys = rms_scaled(raw_keys, key_gain).astype(jnp.bfloat16)
        image_values = jnp.dot(patch_rows, w_value, preferred_element_type=jnp.float32).astype(jnp.bfloat16)
        image_values = image_values.reshape(READS, PATCHES, KV_HEADS, HD)
        first_row = (group_index * per_group).astype(jnp.int32)
        rows_here = lax.dynamic_slice_in_dim(queries, first_row, per_group, 0).astype(jnp.float32)
        normed = rms_scaled(rows_here.reshape(per_group, KV_HEADS, group_size, HD), query_gain).astype(jnp.bfloat16)
        entries = lax.dynamic_slice_in_dim(request_image, first_row, per_group, 0)
        scores = jnp.einsum('bkgd,rskd->bkgrs', normed.astype(jnp.float32), image_keys.astype(jnp.float32)) * scale
        chosen = (entries[:, None] == jnp.arange(READS, dtype=jnp.int32)[None, :]).astype(jnp.float32)
        usable = (jnp.arange(PATCHES, dtype=jnp.int32)[None, :] // TILE_P < image_tiles[images][:, None]).astype(jnp.float32)
        weights = jnp.exp(scores) * chosen[:, None, None, :, None] * usable[None, None, None]
        denominator = lax.optimization_barrier(jnp.sum(weights, axis=(3, 4)))
        numerator = jnp.einsum('bkgrs,rskd->bkgd', weights.astype(jnp.bfloat16).astype(jnp.float32), image_values.astype(jnp.float32))
        return (numerator / denominator[..., None]).astype(jnp.bfloat16).reshape(per_group, HEADS * HD)
    result = lax.map(one_group, jnp.arange(N_WIDE, dtype=jnp.int32))
    return result.reshape(batch, HEADS * HD)
```

```python
import functools
import math

import jax
import jax.numpy as jnp
from jax import lax
from jax.experimental import pallas as pl
from jax.experimental.pallas import tpu as pltpu
from jax.sharding import PartitionSpec as P

HD = 128
EPS = 1e-05
NX = 4
NZH = 4
NZ = 8
SLOTS = NX * NZH
KC = 512
DEPTH = 3
MESH = pl.DeviceIdType.MESH
FAR = (2, 1, 3, 0)


def kernel(
    patches,
    w_key,
    w_value,
    key_gain,
    query_gain,
    queries,
    owner_table,
    reader_table,
    request_image,
    image_tiles,
    out,
    pbuf,
    kbuf,
    vbuf,
    acc,
    kv,
    q_norm,
    q_own,
    code_own,
    q_all,
    code_all,
    num_send,
    den_send,
    num_all,
    den_all,
    fetch_sem,
    kv_send_sem,
    kv_recv_sem,
    q_send_sem,
    q_recv_sem,
    code_send_sem,
    code_recv_sem,
    num_send_sem,
    num_recv_sem,
    den_send_sem,
    den_recv_sem,
):
    images, rows, width = patches.shape
    steps = width // KC
    heads_here = w_key.shape[1] // HD
    group_size = queries.shape[1] // w_key.shape[1]
    wide = lax.axis_index("wide")
    narrow = lax.axis_index("narrow")
    depth = lax.axis_index("depth")
    x, zh = lax.rem(wide, NX), lax.div(wide, NX)
    zl, core = lax.div(depth, 2), lax.rem(depth, 2)
    z = zh * 2 + zl

    def device(x_to, zh_to, zl_to, core_to):
        return (zh_to * NX + x_to, narrow, zl_to * 2 + core_to)

    partner = device(x, zh, zl, 1 - core)

    barrier = pltpu.get_barrier_semaphore()
    for dx in FAR:
        for dz in (4, 3, 5, 2, 6, 1, 7, 0):
            if dx or dz:
                x_to, z_to = lax.rem(x + dx, NX), lax.rem(z + dz, NZ)
                pl.semaphore_signal(
                    barrier,
                    inc=1,
                    device_id=device(x_to, lax.div(z_to, 2), lax.rem(z_to, 2), core),
                    device_id_type=MESH,
                )
    pl.semaphore_signal(barrier, inc=1, device_id=partner, device_id_type=MESH)

    def fetches(step):
        columns = pl.ds(pl.multiple_of(step * KC, KC), KC)
        return (
            pltpu.make_async_copy(patches.at[:, :, columns], pbuf.at[step], fetch_sem.at[0, step]),
            pltpu.make_async_copy(w_key.at[columns, :], kbuf.at[step], fetch_sem.at[1, step]),
            pltpu.make_async_copy(w_value.at[columns, :], vbuf.at[step], fetch_sem.at[2, step]),
        )

    for step in range(DEPTH):
        for copy in fetches(step):
            copy.start()

    mine = queries[...].astype(jnp.float32)
    gain = query_gain[...]
    for head in range(heads_here * group_size):
        part = mine[:, head * HD : (head + 1) * HD]
        mean = jnp.mean(part * part, axis=-1, keepdims=True)
        q_norm[head] = part * lax.rsqrt(mean + EPS) * gain
    for half in range(2):
        for k in range(heads_here):
            own_rows = [
                q_norm[k * group_size + g, pl.ds(8 * half + 4 * core, 4), :]
                for g in range(group_size)
            ]
            q_own[half, k] = jnp.concatenate(own_rows, axis=0).astype(jnp.bfloat16)
    lanes = lax.broadcasted_iota(jnp.int32, (1, HD), 1)
    codes = jnp.zeros((1, HD), jnp.float32)
    for half in range(2):
        for r in range(4):
            image = reader_table[wide, request_image[8 * half + 4 * core + r]]
            code = owner_table[image] * 8 + image_tiles[image]
            codes = jnp.where(lanes == half * 4 + r, code.astype(jnp.float32), codes)
    code_own[...] = codes
    q_all[0] = q_own[...]
    code_all[0] = codes

    def query_copies(d, dx):
        x_to = lax.rem(x + dx, NX)
        z_to = lax.rem(z + NZ + (2 * zl - 1) * d, NZ)
        zh_to = lax.div(z_to, 2)
        slot = dx * NZH + lax.rem(zh_to - zh + NZH, NZH)
        to = device(x_to, zh_to, lax.rem(z_to, 2), core)
        i = d * NX + dx
        return (
            pltpu.make_async_remote_copy(
                src_ref=q_own,
                dst_ref=q_all.at[slot],
                send_sem=q_send_sem.at[i],
                recv_sem=q_recv_sem.at[slot],
                device_id=to,
                device_id_type=MESH,
            ),
            pltpu.make_async_remote_copy(
                src_ref=code_own,
                dst_ref=code_all.at[slot],
                send_sem=code_send_sem.at[i],
                recv_sem=code_recv_sem.at[slot],
                device_id=to,
                device_id_type=MESH,
            ),
        )

    query_order = [(d, dx) for d in (3, 2, 1, 0) for dx in FAR if d or dx]

    def send_queries():
        pl.semaphore_wait(barrier, 2 * SLOTS)
        for d, dx in query_order:
            for copy in query_copies(d, dx):
                copy.start()

    acc[...] = jnp.zeros_like(acc)
    kv_width = heads_here * HD

    def project(step, carry):
        @pl.when(step + DEPTH < steps)
        def _():
            for copy in fetches(step + DEPTH):
                copy.start()

        for copy in fetches(step):
            copy.wait()
        block = pbuf[step].reshape(images * rows, KC)
        acc[:, :kv_width] += jnp.dot(block, kbuf[step], preferred_element_type=jnp.float32)
        acc[:, kv_width:] += jnp.dot(block, vbuf[step], preferred_element_type=jnp.float32)
        return carry

    early = steps // 2
    lax.fori_loop(0, early, project, 0)
    send_queries()
    lax.fori_loop(early, steps, project, 0)

    gain = key_gain[...]
    for k in range(heads_here):
        for j in range(images):
            raw = acc[j * rows : (j + 1) * rows, k * HD : (k + 1) * HD]
            mean = jnp.mean(raw * raw, axis=-1, keepdims=True)
            kv[core, k, 0, :, j * HD : (j + 1) * HD] = (
                raw * lax.rsqrt(mean + EPS) * gain
            ).astype(jnp.bfloat16)
            kv[core, k, 1, :, j * HD : (j + 1) * HD] = acc[
                j * rows : (j + 1) * rows, kv_width + k * HD : kv_width + (k + 1) * HD
            ].astype(jnp.bfloat16)

    def kv_copy(k):
        return pltpu.make_async_remote_copy(
            src_ref=kv.at[core, k],
            dst_ref=kv.at[core, k],
            send_sem=kv_send_sem.at[k],
            recv_sem=kv_recv_sem.at[k],
            device_id=partner,
            device_id_type=MESH,
        )

    for k in range(heads_here):
        kv_copy(k).start()

    def query_arrival(slot):
        return (
            pltpu.make_async_remote_copy(
                src_ref=q_own,
                dst_ref=q_all.at[slot],
                send_sem=q_send_sem.at[0],
                recv_sem=q_recv_sem.at[slot],
                device_id=partner,
                device_id_type=MESH,
            ),
            pltpu.make_async_remote_copy(
                src_ref=code_own,
                dst_ref=code_all.at[slot],
                send_sem=code_send_sem.at[0],
                recv_sem=code_recv_sem.at[slot],
                device_id=partner,
                device_id_type=MESH,
            ),
        )

    for slot in range(1, SLOTS):
        for copy in query_arrival(slot):
            copy.wait_recv()

    per_slot = 2 * group_size * 4
    lane = lax.broadcasted_iota(jnp.int32, (SLOTS, per_slot, HD), 2)
    row = lax.broadcasted_iota(jnp.int32, (SLOTS, per_slot, HD), 1)
    wanted = lax.div(row, 4 * group_size) * 4 + lax.rem(row, 4)
    spread = jnp.where(lane == wanted, jnp.broadcast_to(code_all[...], lane.shape), 0.0)
    total = SLOTS * per_slot
    column = jnp.sum(spread, axis=-1, keepdims=True).reshape(total, 1)
    first_slot = (wide * images * 8).astype(jnp.float32)
    local = jnp.broadcast_to(column, (total, HD)) - first_slot
    tile = (zl * 2).astype(jnp.float32)
    chosen, second = [], jnp.zeros((total, HD), jnp.float32)
    for j in range(images):
        mine_j = (local > 8.0 * j + tile) & (local < 8.0 * j + 7.0)
        chosen.append(jnp.where(mine_j, 1.0, 0.0))
        second = jnp.where((local > 8.0 * j + tile + 1.0) & (local < 8.0 * j + 7.0), 1.0, second)
    any_chosen = chosen[0]
    for j in range(1, images):
        any_chosen = any_chosen + chosen[j]
    chosen16 = [c.astype(jnp.bfloat16) for c in chosen]
    scale = 1.0 / math.sqrt(HD)

    def num_copy(slot, half, k):
        dx, dzh = slot // NZH, slot % NZH
        if slot:
            to_half = half
        else:
            to_half = 1 - zl
        to = device(lax.rem(x - dx + NX, NX), lax.rem(zh - dzh + NZH, NZH), to_half, core)
        return pltpu.make_async_remote_copy(
            src_ref=num_send.at[slot, to_half, k],
            dst_ref=num_all.at[slot * 2 + zl, k],
            send_sem=num_send_sem.at[slot * 2 + half, k],
            recv_sem=num_recv_sem.at[slot * 2 + zl, k],
            device_id=to,
            device_id_type=MESH,
        )

    def den_copy(slot, half):
        dx, dzh = slot // NZH, slot % NZH
        to_half = half if slot else 1 - zl
        to = device(lax.rem(x - dx + NX, NX), lax.rem(zh - dzh + NZH, NZH), to_half, core)
        return pltpu.make_async_remote_copy(
            src_ref=den_send.at[slot * 2 + to_half],
            dst_ref=den_all.at[slot * 2 + zl],
            send_sem=den_send_sem.at[slot * 2 + half],
            recv_sem=den_recv_sem.at[slot * 2 + zl],
            device_id=to,
            device_id_type=MESH,
        )

    return_order = [
        (dx * NZH + dzh, half)
        for dzh in FAR
        for dx in FAR
        for half in range(2 if dx or dzh else 1)
    ]

    chunk = group_size * 4
    lane3 = lax.broadcasted_iota(jnp.int32, (2 * SLOTS, chunk, HD), 2)
    row3 = lax.broadcasted_iota(jnp.int32, (2 * SLOTS, chunk, HD), 1)
    dens = jnp.zeros((2 * SLOTS, 1, HD), jnp.float32)
    for k in range(heads_here):
        kv_copy(k).wait_recv()
        q = q_all[:, :, k].reshape(total, HD)
        expanded = jnp.concatenate([q * chosen16[j] for j in range(images)], axis=-1)
        keys = kv[:, k, 0].reshape(2 * rows, images * HD)
        scores = lax.dot_general(
            expanded, keys, (((1,), (1,)), ((), ())), preferred_element_type=jnp.float32
        )
        weights = jnp.exp(scores * scale)
        w0 = weights[:, :rows]
        w1 = weights[:, rows:] * jnp.concatenate([second] * (rows // HD), axis=-1)
        both = w0 + w1
        folded = both[:, :HD]
        for i in range(1, rows // HD):
            folded = folded + both[:, i * HD : (i + 1) * HD]
        den = jnp.sum(folded, axis=-1, keepdims=True)
        values = kv[:, k, 1].reshape(2 * rows, images * HD)
        pulled = jnp.dot(
            jnp.concatenate([w0, w1], axis=-1).astype(jnp.bfloat16),
            values,
            preferred_element_type=jnp.float32,
        )
        num = pulled[:, :HD] * chosen[0]
        for j in range(1, images):
            num = num + pulled[:, j * HD : (j + 1) * HD] * chosen[j]
        num_send[:, :, k] = num.astype(jnp.bfloat16).reshape(SLOTS, 2, chunk, HD)
        for slot, half in return_order:
            num_copy(slot, half, k).start()
        den = jnp.broadcast_to(den, (total, HD)) * any_chosen
        den = den.reshape(2 * SLOTS, chunk, HD)
        dens = dens + jnp.sum(
            jnp.where(lane3 == row3 + k * chunk, den, 0.0), axis=1, keepdims=True
        )
    den_send[...] = dens
    for slot, half in return_order:
        den_copy(slot, half).start()
    num_all[zl] = num_send[0, zl]
    den_all[zl] = den_send[zl]

    for k in range(heads_here):
        for slot, half in return_order:
            pltpu.make_async_remote_copy(
                src_ref=num_send.at[slot, half, k],
                dst_ref=num_all.at[slot * 2 + (half if slot else 1 - zl), k],
                send_sem=num_send_sem.at[slot * 2 + half, k],
                recv_sem=num_recv_sem.at[slot * 2 + (half if slot else 1 - zl), k],
                device_id=partner,
                device_id_type=MESH,
            ).wait_recv()
    for slot, half in return_order:
        pltpu.make_async_remote_copy(
            src_ref=den_send.at[slot * 2 + half],
            dst_ref=den_all.at[slot * 2 + (half if slot else 1 - zl)],
            send_sem=den_send_sem.at[slot * 2 + half],
            recv_sem=den_recv_sem.at[slot * 2 + (half if slot else 1 - zl)],
            device_id=partner,
            device_id_type=MESH,
        ).wait_recv()

    den_total = jnp.sum(den_all[...], axis=0)
    pair_rows = heads_here * chunk
    lane2 = lax.broadcasted_iota(jnp.int32, (pair_rows, HD), 1)
    row2 = lax.broadcasted_iota(jnp.int32, (pair_rows, HD), 0)
    den_column = jnp.sum(
        jnp.where(lane2 == row2, jnp.broadcast_to(den_total, (pair_rows, HD)), 0.0),
        axis=-1,
        keepdims=True,
    )
    num_total = jnp.sum(num_all[...].astype(jnp.float32), axis=0).reshape(pair_rows, HD)
    context = num_total / den_column
    for head in range(heads_here * group_size):
        out[:, head * HD : (head + 1) * HD] = context[head * 4 : (head + 1) * 4, :].astype(
            jnp.bfloat16
        )

    for d, dx in query_order:
        for copy in query_copies(d, dx):
            copy.wait_send()
    for k in range(heads_here):
        kv_copy(k).wait_send()
        for slot, half in return_order:
            num_copy(slot, half, k).wait_send()
    for slot, half in return_order:
        den_copy(slot, half).wait_send()


def local(
    patch_store,
    w_key,
    w_value,
    key_gain,
    query_gain,
    queries,
    owner_table,
    reader_table,
    request_image,
    image_tiles,
):
    images, rows, width = patch_store.shape
    kv_width = w_key.shape[1]
    heads_here = kv_width // HD
    group_size = queries.shape[1] // kv_width
    batch_here = queries.shape[0]
    steps = width // KC
    chunk = group_size * 4
    vmem = pl.BlockSpec(memory_space=pltpu.VMEM)
    smem = pl.BlockSpec(memory_space=pltpu.SMEM)
    hbm = pl.BlockSpec(memory_space=pl.ANY)
    dma = pltpu.SemaphoreType.DMA
    return pl.pallas_call(
        kernel,
        out_shape=jax.ShapeDtypeStruct((4, queries.shape[1]), jnp.bfloat16),
        in_specs=[hbm] * 3 + [vmem] * 3 + [smem] * 4,
        out_specs=vmem,
        scratch_shapes=[
            pltpu.VMEM((steps, images, rows, KC), jnp.bfloat16),
            pltpu.VMEM((steps, KC, kv_width), jnp.bfloat16),
            pltpu.VMEM((steps, KC, kv_width), jnp.bfloat16),
            pltpu.VMEM((images * rows, 2 * kv_width), jnp.float32),
            pltpu.VMEM((2, heads_here, 2, rows, images * HD), jnp.bfloat16),
            pltpu.VMEM((heads_here * group_size, batch_here, HD), jnp.float32),
            pltpu.VMEM((2, heads_here, chunk, HD), jnp.bfloat16),
            pltpu.VMEM((1, HD), jnp.float32),
            pltpu.VMEM((SLOTS, 2, heads_here, chunk, HD), jnp.bfloat16),
            pltpu.VMEM((SLOTS, 1, HD), jnp.float32),
            pltpu.VMEM((SLOTS, 2, heads_here, chunk, HD), jnp.bfloat16),
            pltpu.VMEM((2 * SLOTS, 1, HD), jnp.float32),
            pltpu.VMEM((2 * SLOTS, heads_here, chunk, HD), jnp.bfloat16),
            pltpu.VMEM((2 * SLOTS, 1, HD), jnp.float32),
            dma((3, steps)),
            dma((heads_here,)),
            dma((heads_here,)),
            dma((SLOTS,)),
            dma((SLOTS,)),
            dma((SLOTS,)),
            dma((SLOTS,)),
            dma((2 * SLOTS, heads_here)),
            dma((2 * SLOTS, heads_here)),
            dma((2 * SLOTS,)),
            dma((2 * SLOTS,)),
        ],
        compiler_params=pltpu.CompilerParams(
            collective_id=0, has_side_effects=True, vmem_limit_bytes=56 * 1024 * 1024
        ),
        name="attend",
    )(
        patch_store,
        w_key,
        w_value,
        key_gain[None],
        query_gain[None],
        queries,
        owner_table,
        reader_table,
        request_image,
        image_tiles,
    )


def solution(mesh):
    placed = (
        P("wide", "depth", None),
        P(None, "narrow"),
        P(None, "narrow"),
        P(),
        P(),
        P("wide", "narrow"),
        P(),
        P(),
        P("wide"),
        P(),
    )
    return jax.shard_map(
        local, mesh=mesh, in_specs=placed, out_specs=P(("wide", "depth"), "narrow"), check_vma=False
    )
```

```python
import math

import jax
import jax.numpy as jnp
from jax import lax
from jax.experimental import pallas as pl
from jax.experimental.pallas import tpu as pltpu
from jax.sharding import PartitionSpec as P

HD = 128
EPS = 1e-05
NX = 4
NZH = 4
NZ = 8
SLOTS = NX * NZH
NEAR = 3 * NX
KC = 512
WC = 1024
MESH = pl.DeviceIdType.MESH
FAR = (2, 1, 3, 0)


def kernel(
    patches,
    w_key,
    w_value,
    key_gain_in,
    query_gain_in,
    queries_in,
    owner_in,
    reader_in,
    request_in,
    tiles_in,
    out,
    pbuf,
    kbuf,
    vbuf,
    acc_k,
    acc_v,
    kv,
    queries,
    key_gain,
    query_gain,
    owner_table,
    reader_table,
    request_image,
    image_tiles,
    q_norm,
    q_own,
    code_own,
    q_all,
    code_all,
    num_send,
    den_send,
    num_all,
    den_all,
    small_sem,
    patch_sem,
    weight_sem,
    kv_sem,
    q_sem,
    code_sem,
    num_sem,
    den_sem,
):
    images, rows, width = patches.shape
    steps = width // KC
    kv_width = w_key.shape[1]
    heads_here = kv_width // HD
    group_size = queries.shape[1] // kv_width
    wide = lax.axis_index("wide")
    narrow = lax.axis_index("narrow")
    depth = lax.axis_index("depth")
    x, zh = lax.rem(wide, NX), lax.div(wide, NX)
    zl, core = lax.div(depth, 2), lax.rem(depth, 2)
    z = zh * 2 + zl

    def device(x_to, zh_to, zl_to, core_to):
        return (zh_to * NX + x_to, narrow, zl_to * 2 + core_to)

    partner = device(x, zh, zl, 1 - core)

    barrier = pltpu.get_barrier_semaphore()
    for dz in (4, 3, 5, 2, 6, 1, 7, 0):
        for dx in FAR:
            if dx or dz:
                x_to, z_to = lax.rem(x + dx, NX), lax.rem(z + dz, NZ)
                pl.semaphore_signal(
                    barrier,
                    inc=1,
                    device_id=device(x_to, lax.div(z_to, 2), lax.rem(z_to, 2), core),
                    device_id_type=MESH,
                )
    pl.semaphore_signal(barrier, inc=1, device_id=partner, device_id_type=MESH)

    small = [
        pltpu.make_async_copy(source, target, small_sem.at[i])
        for i, (source, target) in enumerate(
            (
                (queries_in, queries),
                (query_gain_in, query_gain),
                (request_in, request_image),
                (reader_in, reader_table),
                (owner_in, owner_table),
                (tiles_in, image_tiles),
                (key_gain_in, key_gain),
            )
        )
    ]
    for copy in small:
        copy.start()

    def fetch_patches(step):
        return pltpu.make_async_copy(
            patches.at[:, :, pl.ds(step * KC, KC)], pbuf.at[step], patch_sem.at[step]
        )

    def fetch_weight(which, part):
        source, target = ((w_key, kbuf), (w_value, vbuf))[which]
        span = pl.ds(part * WC, WC)
        return pltpu.make_async_copy(
            source.at[span, :], target.at[span, :], weight_sem.at[which, part]
        )

    both = steps // 2
    per = WC // KC
    fetches = []
    for step in range(steps):
        if step % per == 0:
            fetches.append([fetch_weight(0, step // per)])
            if step < both:
                fetches[-1].append(fetch_weight(1, step // per))
        else:
            fetches.append([])
        fetches[-1].append(fetch_patches(step))
    for part in range(both // per, steps // per):
        fetches[steps - 1].append(fetch_weight(1, part))

    ahead = 4
    for step in range(ahead):
        for copy in fetches[step]:
            copy.start()

    small[0].wait()
    small[1].wait()
    mine = queries[...].astype(jnp.float32)
    gain = query_gain[...]
    for head in range(heads_here * group_size):
        part = mine[:, head * HD : (head + 1) * HD]
        mean = jnp.mean(part * part, axis=-1, keepdims=True)
        q_norm[head] = part * lax.rsqrt(mean + EPS) * gain
    for half in range(2):
        for k in range(heads_here):
            own_rows = [
                q_norm[k * group_size + g, pl.ds(8 * half + 4 * core, 4), :]
                for g in range(group_size)
            ]
            q_own[half, k] = jnp.concatenate(own_rows, axis=0).astype(jnp.bfloat16)
    lanes = lax.broadcasted_iota(jnp.int32, (1, HD), 1)
    codes = jnp.zeros((1, HD), jnp.float32)
    for copy in small[2:]:
        copy.wait()
    for half in range(2):
        for r in range(4):
            image = reader_table[request_image[8 * half + 4 * core + r], wide]
            code = owner_table[image] * 8 + image_tiles[image]
            codes = jnp.where(lanes == half * 4 + r, code.astype(jnp.float32), codes)
    code_own[...] = codes
    q_all[0] = q_own[...]
    code_all[0] = codes

    def query_copies(d, dx):
        x_to = lax.rem(x + dx, NX)
        z_to = lax.rem(z + NZ + (2 * zl - 1) * d, NZ)
        zh_to = lax.div(z_to, 2)
        dzh = lax.rem(zh_to - zh + NZH, NZH)
        place = jnp.where(dzh == 2, 3, jnp.where(dzh == 3, 2, dzh))
        slot = place * NX + dx
        to = device(x_to, zh_to, lax.rem(z_to, 2), core)
        far = 1 if d == 3 else 0
        return (
            pltpu.make_async_remote_copy(
                src_ref=q_own,
                dst_ref=q_all.at[slot],
                send_sem=q_sem.at[0],
                recv_sem=q_sem.at[1 + far],
                device_id=to,
                device_id_type=MESH,
            ),
            pltpu.make_async_remote_copy(
                src_ref=code_own,
                dst_ref=code_all.at[slot],
                send_sem=code_sem.at[0],
                recv_sem=code_sem.at[1 + far],
                device_id=to,
                device_id_type=MESH,
            ),
        )

    def send_queries():
        pl.semaphore_wait(barrier, 2 * SLOTS)
        for d in (3, 2, 1, 0):
            for dx in FAR:
                if d or dx:
                    for copy in query_copies(d, dx):
                        copy.start()

    def settle(ref, sem):
        pltpu.make_async_copy(ref, ref, sem).wait()

    def project(acc, weight, step):
        block = pbuf[step].reshape(images * rows, KC)
        product = jnp.dot(
            block, weight[step * KC : (step + 1) * KC, :], preferred_element_type=jnp.float32
        )
        if step == 0:
            acc[...] = product
        else:
            acc[...] += product

    for step in range(steps):
        if step + ahead < steps:
            for copy in fetches[step + ahead]:
                copy.start()
        if step % per == 0:
            fetch_weight(0, step // per).wait()
            if step < both:
                fetch_weight(1, step // per).wait()
        fetch_patches(step).wait()
        project(acc_k, kbuf, step)
        if step < both:
            project(acc_v, vbuf, step)
        if step == 1:
            send_queries()

    def swap(which):
        return pltpu.make_async_remote_copy(
            src_ref=kv.at[which, core],
            dst_ref=kv.at[which, core],
            send_sem=kv_sem.at[which],
            recv_sem=kv_sem.at[2 + which],
            device_id=partner,
            device_id_type=MESH,
        )

    gain = key_gain[...]
    for k in range(heads_here):
        for j in range(images):
            raw = acc_k[j * rows : (j + 1) * rows, k * HD : (k + 1) * HD]
            mean = jnp.mean(raw * raw, axis=-1, keepdims=True)
            kv[0, core, k, :, j * HD : (j + 1) * HD] = (
                raw * lax.rsqrt(mean + EPS) * gain
            ).astype(jnp.bfloat16)
    swap(0).start()
    for step in range(both, steps):
        if step % per == 0:
            fetch_weight(1, step // per).wait()
        project(acc_v, vbuf, step)
    for k in range(heads_here):
        for j in range(images):
            kv[1, core, k, :, j * HD : (j + 1) * HD] = acc_v[
                j * rows : (j + 1) * rows, k * HD : (k + 1) * HD
            ].astype(jnp.bfloat16)
    swap(1).start()

    chunk = group_size * 4
    per_slot = 2 * chunk
    scale = 1.0 / math.sqrt(HD)
    first_slot = (wide * images * 8).astype(jnp.float32)
    tile = (zl * 2).astype(jnp.float32)

    def return_copies(slot, half):
        place, dx = slot // NX, slot % NX
        dzh = (0, 1, 3, 2)[place]
        to_half = half if slot else 1 - zl
        to = device(lax.rem(x - dx + NX, NX), lax.rem(zh - dzh + NZH, NZH), to_half, core)
        return (
            pltpu.make_async_remote_copy(
                src_ref=num_send.at[slot, to_half],
                dst_ref=num_all.at[slot * 2 + zl],
                send_sem=num_sem.at[0],
                recv_sem=num_sem.at[1],
                device_id=to,
                device_id_type=MESH,
            ),
            pltpu.make_async_remote_copy(
                src_ref=den_send.at[slot * 2 + to_half],
                dst_ref=den_all.at[slot * 2 + zl],
                send_sem=den_sem.at[0],
                recv_sem=den_sem.at[1],
                device_id=to,
                device_id_type=MESH,
            ),
        )

    def attend(first, last):
        count = last - first
        total = count * per_slot
        lane = lax.broadcasted_iota(jnp.int32, (count, per_slot, HD), 2)
        row = lax.broadcasted_iota(jnp.int32, (count, per_slot, HD), 1)
        wanted = lax.div(row, chunk) * 4 + lax.rem(row, 4)
        spread = jnp.where(
            lane == wanted, jnp.broadcast_to(code_all[first:last], lane.shape), 0.0
        )
        column = jnp.sum(spread, axis=-1, keepdims=True).reshape(total, 1)
        local = jnp.broadcast_to(column, (total, HD)) - first_slot
        chosen, second = [], jnp.zeros((total, HD), jnp.float32)
        for j in range(images):
            below = local < 8.0 * j + 7.0
            chosen.append(jnp.where((local > 8.0 * j + tile) & below, 1.0, 0.0))
            second = jnp.where((local > 8.0 * j + tile + 1.0) & below, 1.0, second)
        any_chosen = chosen[0]
        for j in range(1, images):
            any_chosen = any_chosen + chosen[j]
        lane3 = lax.broadcasted_iota(jnp.int32, (2 * count, chunk, HD), 2)
        row3 = lax.broadcasted_iota(jnp.int32, (2 * count, chunk, HD), 1)
        dens = jnp.zeros((2 * count, 1, HD), jnp.float32)
        all_weights = []
        for k in range(heads_here):
            q = q_all[first:last, :, k].reshape(total, HD)
            expanded = jnp.concatenate(
                [q * chosen[j].astype(jnp.bfloat16) for j in range(images)], axis=-1
            )
            if first == 0 and k == 0:
                swap(0).wait_recv()
            keys = kv[0, :, k].reshape(2 * rows, images * HD)
            scores = lax.dot_general(
                expanded, keys, (((1,), (1,)), ((), ())), preferred_element_type=jnp.float32
            )
            weights = jnp.exp(scores * scale)
            w0 = weights[:, :rows]
            w1 = weights[:, rows:] * jnp.concatenate([second] * (rows // HD), axis=-1)
            summed = w0 + w1
            folded = summed[:, :HD]
            for i in range(1, rows // HD):
                folded = folded + summed[:, i * HD : (i + 1) * HD]
            den = jnp.sum(folded, axis=-1, keepdims=True)
            den = (jnp.broadcast_to(den, (total, HD)) * any_chosen).reshape(2 * count, chunk, HD)
            dens = dens + jnp.sum(
                jnp.where(lane3 == row3 + k * chunk, den, 0.0), axis=1, keepdims=True
            )
            all_weights.append(jnp.concatenate([w0, w1], axis=-1).astype(jnp.bfloat16))
        den_send[2 * first : 2 * last] = dens
        if first == 0:
            swap(1).wait_recv()
        for k in range(heads_here):
            values = kv[1, :, k].reshape(2 * rows, images * HD)
            pulled = jnp.dot(all_weights[k], values, preferred_element_type=jnp.float32)
            num = pulled[:, :HD] * chosen[0]
            for j in range(1, images):
                num = num + pulled[:, j * HD : (j + 1) * HD] * chosen[j]
            num_send[first:last, :, k] = num.astype(jnp.bfloat16).reshape(count, 2, chunk, HD)
        for place in reversed(range(first // NX, last // NX)):
            for dx in FAR:
                slot = place * NX + dx
                for half in range(2 if slot else 1):
                    for copy in return_copies(slot, half):
                        copy.start()

    settle(q_all.at[1:NEAR], q_sem.at[1])
    settle(code_all.at[1:NEAR], code_sem.at[1])
    attend(0, NEAR)
    settle(q_all.at[NEAR:SLOTS], q_sem.at[2])
    settle(code_all.at[NEAR:SLOTS], code_sem.at[2])
    attend(NEAR, SLOTS)
    num_all[zl] = num_send[0, zl]
    den_all[zl] = den_send[zl]

    settle(q_all.at[1:SLOTS], q_sem.at[0])
    settle(code_all.at[1:SLOTS], code_sem.at[0])
    swap(0).wait_send()
    swap(1).wait_send()
    settle(num_all.at[1 : 2 * SLOTS], num_sem.at[0])
    settle(den_all.at[1 : 2 * SLOTS], den_sem.at[0])
    settle(den_all.at[1 : 2 * SLOTS], den_sem.at[1])
    settle(num_all.at[1 : 2 * SLOTS], num_sem.at[1])

    den_total = jnp.sum(den_all[...], axis=0)
    pair_rows = heads_here * chunk
    lane2 = lax.broadcasted_iota(jnp.int32, (pair_rows, HD), 1)
    row2 = lax.broadcasted_iota(jnp.int32, (pair_rows, HD), 0)
    den_column = jnp.sum(
        jnp.where(lane2 == row2, jnp.broadcast_to(den_total, (pair_rows, HD)), 0.0),
        axis=-1,
        keepdims=True,
    )
    num_total = jnp.sum(num_all[...].astype(jnp.float32), axis=0).reshape(pair_rows, HD)
    context = num_total / den_column
    for head in range(heads_here * group_size):
        out[:, head * HD : (head + 1) * HD] = context[head * 4 : (head + 1) * 4, :].astype(
            jnp.bfloat16
        )


def local(
    patch_store,
    w_key,
    w_value,
    key_gain,
    query_gain,
    queries,
    owner_table,
    reader_table,
    request_image,
    image_tiles,
):
    images, rows, width = patch_store.shape
    kv_width = w_key.shape[1]
    heads_here = kv_width // HD
    group_size = queries.shape[1] // kv_width
    steps = width // KC
    chunk = group_size * 4
    groups, reads = reader_table.shape
    vmem = pl.BlockSpec(memory_space=pltpu.VMEM)
    hbm = pl.BlockSpec(memory_space=pl.ANY)
    dma = pltpu.SemaphoreType.DMA
    return pl.pallas_call(
        kernel,
        out_shape=jax.ShapeDtypeStruct((4, queries.shape[1]), jnp.bfloat16),
        in_specs=[hbm] * 10,
        out_specs=vmem,
        scratch_shapes=[
            pltpu.VMEM((steps, images, rows, KC), jnp.bfloat16),
            pltpu.VMEM((width, kv_width), jnp.bfloat16),
            pltpu.VMEM((width, kv_width), jnp.bfloat16),
            pltpu.VMEM((images * rows, kv_width), jnp.float32),
            pltpu.VMEM((images * rows, kv_width), jnp.float32),
            pltpu.VMEM((2, 2, heads_here, rows, images * HD), jnp.bfloat16),
            pltpu.VMEM(queries.shape, jnp.bfloat16),
            pltpu.VMEM((1, HD), jnp.float32),
            pltpu.VMEM((1, HD), jnp.float32),
            pltpu.SMEM(owner_table.shape, jnp.int32),
            pltpu.SMEM((reads, groups), jnp.int32),
            pltpu.SMEM(request_image.shape, jnp.int32),
            pltpu.SMEM(image_tiles.shape, jnp.int32),
            pltpu.VMEM((heads_here * group_size, queries.shape[0], HD), jnp.float32),
            pltpu.VMEM((2, heads_here, chunk, HD), jnp.bfloat16),
            pltpu.VMEM((1, HD), jnp.float32),
            pltpu.VMEM((SLOTS, 2, heads_here, chunk, HD), jnp.bfloat16),
            pltpu.VMEM((SLOTS, 1, HD), jnp.float32),
            pltpu.VMEM((SLOTS, 2, heads_here, chunk, HD), jnp.bfloat16),
            pltpu.VMEM((2 * SLOTS, 1, HD), jnp.float32),
            pltpu.VMEM((2 * SLOTS, heads_here, chunk, HD), jnp.bfloat16),
            pltpu.VMEM((2 * SLOTS, 1, HD), jnp.float32),
            dma((7,)),
            dma((steps,)),
            dma((2, width // WC)),
            dma((4,)),
            dma((3,)),
            dma((3,)),
            dma((2,)),
            dma((2,)),
        ],
        compiler_params=pltpu.CompilerParams(
            collective_id=0, has_side_effects=True, vmem_limit_bytes=56 * 1024 * 1024
        ),
        name="attend",
    )(
        patch_store,
        w_key,
        w_value,
        key_gain[None],
        query_gain[None],
        queries,
        owner_table,
        reader_table.T,
        request_image,
        image_tiles,
    )


def solution(mesh):
    placed = (
        P("wide", "depth", None),
        P(None, "narrow"),
        P(None, "narrow"),
        P(),
        P(),
        P("wide", "narrow"),
        P(),
        P(),
        P("wide"),
        P(),
    )
    return jax.shard_map(
        local, mesh=mesh, in_specs=placed, out_specs=P(("wide", "depth"), "narrow"), check_vma=False
    )
```

```python
import math

import jax
import jax.numpy as jnp
from jax import lax
from jax.experimental import pallas as pl
from jax.experimental.pallas import tpu as pltpu
from jax.sharding import PartitionSpec as P

HD = 128
EPS = 1e-05
NX = 4
NZH = 4
NZ = 8
SHIFTS = (0, 1, 3, 2)
OWN, NEAR, AWAY = (0, 1), (1, 3), (3, 4)
KC = 512
WC = 1024
MESH = pl.DeviceIdType.MESH


def kernel(
    patches,
    w_key,
    w_value,
    key_gain_in,
    query_gain_in,
    queries_in,
    owner_in,
    reader_in,
    request_in,
    tiles_in,
    out,
    pbuf,
    kbuf,
    vbuf,
    acc_k,
    acc_v,
    kv,
    queries,
    key_gain,
    query_gain,
    owner_table,
    reader_table,
    request_image,
    image_tiles,
    q_norm,
    q_own,
    code_own,
    q_all,
    code_all,
    num_send,
    den_send,
    num_x,
    den_x,
    num_pass,
    den_pass,
    num_z,
    den_z,
    small_sem,
    patch_sem,
    weight_sem,
    kv_sem,
    q_sem,
    code_sem,
    num_sem,
    den_sem,
):
    images, rows, width = patches.shape
    steps = width // KC
    kv_width = w_key.shape[1]
    heads_here = kv_width // HD
    group_size = queries.shape[1] // kv_width
    wide = lax.axis_index("wide")
    narrow = lax.axis_index("narrow")
    depth = lax.axis_index("depth")
    x, zh = lax.rem(wide, NX), lax.div(wide, NX)
    zl, core = lax.div(depth, 2), lax.rem(depth, 2)
    z = zh * 2 + zl

    def device(x_to, zh_to, zl_to, core_to):
        return (zh_to * NX + x_to, narrow, zl_to * 2 + core_to)

    partner = device(x, zh, zl, 1 - core)

    barrier = pltpu.get_barrier_semaphore()
    for dz in (4, 3, 5, 2, 6, 1, 7):
        z_to = lax.rem(z + dz, NZ)
        pl.semaphore_signal(
            barrier,
            inc=1,
            device_id=device(x, lax.div(z_to, 2), lax.rem(z_to, 2), core),
            device_id_type=MESH,
        )
    for dx in (2, 1, 3):
        pl.semaphore_signal(
            barrier,
            inc=1,
            device_id=device(lax.rem(x + dx, NX), zh, zl, core),
            device_id_type=MESH,
        )
    pl.semaphore_signal(barrier, inc=1, device_id=partner, device_id_type=MESH)

    small = [
        pltpu.make_async_copy(source, target, small_sem.at[i])
        for i, (source, target) in enumerate(
            (
                (queries_in, queries),
                (query_gain_in, query_gain),
                (request_in, request_image),
                (reader_in, reader_table),
                (owner_in, owner_table),
                (tiles_in, image_tiles),
                (key_gain_in, key_gain),
            )
        )
    ]
    for copy in small:
        copy.start()

    def fetch_patches(step):
        return pltpu.make_async_copy(
            patches.at[:, :, pl.ds(step * KC, KC)], pbuf.at[step], patch_sem.at[step]
        )

    def fetch_weight(which, part):
        source, target = ((w_key, kbuf), (w_value, vbuf))[which]
        span = pl.ds(part * WC, WC)
        return pltpu.make_async_copy(
            source.at[span, :], target.at[span, :], weight_sem.at[which, part]
        )

    both = steps // 2
    per = WC // KC
    fetches = []
    for step in range(steps):
        if step % per == 0:
            fetches.append([fetch_weight(0, step // per)])
            if step < both:
                fetches[-1].append(fetch_weight(1, step // per))
        else:
            fetches.append([])
        fetches[-1].append(fetch_patches(step))
    for part in range(both // per, steps // per):
        fetches[steps - 1].append(fetch_weight(1, part))

    ahead = 4
    for step in range(ahead):
        for copy in fetches[step]:
            copy.start()

    small[0].wait()
    small[1].wait()
    mine = queries[...].astype(jnp.float32)
    gain = query_gain[...]
    for head in range(heads_here * group_size):
        part = mine[:, head * HD : (head + 1) * HD]
        mean = jnp.mean(part * part, axis=-1, keepdims=True)
        q_norm[head] = part * lax.rsqrt(mean + EPS) * gain
    for half in range(2):
        for k in range(heads_here):
            own_rows = [
                q_norm[k * group_size + g, pl.ds(8 * half + 4 * core, 4), :]
                for g in range(group_size)
            ]
            q_own[half, k] = jnp.concatenate(own_rows, axis=0).astype(jnp.bfloat16)
    lanes = lax.broadcasted_iota(jnp.int32, (1, HD), 1)
    codes = jnp.zeros((1, HD), jnp.float32)
    for copy in small[2:]:
        copy.wait()
    for half in range(2):
        for r in range(4):
            image = reader_table[request_image[8 * half + 4 * core + r], wide]
            code = owner_table[image] * 8 + image_tiles[image]
            codes = jnp.where(lanes == half * 4 + r, code.astype(jnp.float32), codes)
    code_own[...] = codes
    q_all[0, 0] = q_own[...]
    code_all[0, 0] = codes

    def pair(sources, targets, send, recv, to):
        return [
            pltpu.make_async_remote_copy(
                src_ref=source,
                dst_ref=target,
                send_sem=sems.at[send],
                recv_sem=sems.at[recv],
                device_id=to,
                device_id_type=MESH,
            )
            for source, target, sems in zip(sources, targets, (q_sem, code_sem))
        ]

    def start(copies):
        for copy in copies:
            copy.start()

    def send_queries():
        pl.semaphore_wait(barrier, NZ - 1 + NX - 1 + 1)
        for d in (3, 2, 1):
            z_to = lax.rem(z + NZ + (2 * zl - 1) * d, NZ)
            zh_to = lax.div(z_to, 2)
            dzh = lax.rem(zh_to - zh + NZH, NZH)
            place = jnp.where(dzh == 2, 3, jnp.where(dzh == 3, 2, dzh))
            start(
                pair(
                    (q_own, code_own),
                    (q_all.at[0, place], code_all.at[0, place]),
                    0,
                    4 if d == 3 else 5,
                    device(x, zh_to, lax.rem(z_to, 2), core),
                )
            )
        for dx in (2, 1, 3):
            start(
                pair(
                    (q_own, code_own),
                    (q_all.at[dx, 0], code_all.at[dx, 0]),
                    1,
                    6,
                    device(lax.rem(x + dx, NX), zh, zl, core),
                )
            )

    def pass_queries(places, send, recv):
        span = slice(*places)
        for dx in (2, 1, 3):
            start(
                pair(
                    (q_all.at[0, span], code_all.at[0, span]),
                    (q_all.at[dx, span], code_all.at[dx, span]),
                    send,
                    recv,
                    device(lax.rem(x + dx, NX), zh, zl, core),
                )
            )

    def settle_queries(where, index):
        settle(q_all.at[where], q_sem.at[index])
        settle(code_all.at[where], code_sem.at[index])

    def settle(ref, sem):
        pltpu.make_async_copy(ref, ref, sem).wait()

    def project(acc, weight, step):
        block = pbuf[step].reshape(images * rows, KC)
        product = jnp.dot(
            block, weight[step * KC : (step + 1) * KC, :], preferred_element_type=jnp.float32
        )
        if step == 0:
            acc[...] = product
        else:
            acc[...] += product

    for step in range(steps):
        if step + ahead < steps:
            for copy in fetches[step + ahead]:
                copy.start()
        if step % per == 0:
            fetch_weight(0, step // per).wait()
            if step < both:
                fetch_weight(1, step // per).wait()
        fetch_patches(step).wait()
        project(acc_k, kbuf, step)
        if step < both:
            project(acc_v, vbuf, step)
        if step == 1:
            send_queries()

    def swap(which):
        return pltpu.make_async_remote_copy(
            src_ref=kv.at[which, core],
            dst_ref=kv.at[which, core],
            send_sem=kv_sem.at[which],
            recv_sem=kv_sem.at[2 + which],
            device_id=partner,
            device_id_type=MESH,
        )

    gain = key_gain[...]
    for k in range(heads_here):
        for j in range(images):
            raw = acc_k[j * rows : (j + 1) * rows, k * HD : (k + 1) * HD]
            mean = jnp.mean(raw * raw, axis=-1, keepdims=True)
            kv[0, core, k, :, j * HD : (j + 1) * HD] = (
                raw * lax.rsqrt(mean + EPS) * gain
            ).astype(jnp.bfloat16)
    swap(0).start()
    for step in range(both, steps):
        if step % per == 0:
            fetch_weight(1, step // per).wait()
        project(acc_v, vbuf, step)
    for k in range(heads_here):
        for j in range(images):
            kv[1, core, k, :, j * HD : (j + 1) * HD] = acc_v[
                j * rows : (j + 1) * rows, k * HD : (k + 1) * HD
            ].astype(jnp.bfloat16)
    swap(1).start()

    chunk = group_size * 4
    per_slot = 2 * chunk
    scale = 1.0 / math.sqrt(HD)
    first_slot = (wide * images * 8).astype(jnp.float32)
    tile = (zl * 2).astype(jnp.float32)

    def return_pair(sources, targets, send, recv, to):
        return [
            pltpu.make_async_remote_copy(
                src_ref=source,
                dst_ref=target,
                send_sem=sems.at[send],
                recv_sem=sems.at[recv],
                device_id=to,
                device_id_type=MESH,
            )
            for source, target, sems in zip(sources, targets, (num_sem, den_sem))
        ]

    def settle_return(num, den, index):
        settle(num, num_sem.at[index])
        settle(den, den_sem.at[index])

    def attend(places, index, opening):
        span = slice(*places)
        count = NX * (places[1] - places[0])
        total = count * per_slot
        lane = lax.broadcasted_iota(jnp.int32, (count, per_slot, HD), 2)
        row = lax.broadcasted_iota(jnp.int32, (count, per_slot, HD), 1)
        wanted = lax.div(row, chunk) * 4 + lax.rem(row, 4)
        spread = jnp.where(
            lane == wanted, jnp.broadcast_to(code_all[:, span].reshape(count, 1, HD), lane.shape), 0.0
        )
        column = jnp.sum(spread, axis=-1, keepdims=True).reshape(total, 1)
        local = jnp.broadcast_to(column, (total, HD)) - first_slot
        chosen, second = [], jnp.zeros((total, HD), jnp.float32)
        for j in range(images):
            below = local < 8.0 * j + 7.0
            chosen.append(jnp.where((local > 8.0 * j + tile) & below, 1.0, 0.0))
            second = jnp.where((local > 8.0 * j + tile + 1.0) & below, 1.0, second)
        any_chosen = chosen[0]
        for j in range(1, images):
            any_chosen = any_chosen + chosen[j]
        lane3 = lax.broadcasted_iota(jnp.int32, (2 * count, chunk, HD), 2)
        row3 = lax.broadcasted_iota(jnp.int32, (2 * count, chunk, HD), 1)
        dens = jnp.zeros((2 * count, 1, HD), jnp.float32)
        all_weights = []
        for k in range(heads_here):
            q = q_all[:, span, :, k].reshape(total, HD)
            expanded = jnp.concatenate(
                [q * chosen[j].astype(jnp.bfloat16) for j in range(images)], axis=-1
            )
            if opening and k == 0:
                swap(0).wait_recv()
            keys = kv[0, :, k].reshape(2 * rows, images * HD)
            scores = lax.dot_general(
                expanded, keys, (((1,), (1,)), ((), ())), preferred_element_type=jnp.float32
            )
            weights = jnp.exp(scores * scale)
            w0 = weights[:, :rows]
            w1 = weights[:, rows:] * jnp.concatenate([second] * (rows // HD), axis=-1)
            summed = w0 + w1
            folded = summed[:, :HD]
            for i in range(1, rows // HD):
                folded = folded + summed[:, i * HD : (i + 1) * HD]
            den = jnp.sum(folded, axis=-1, keepdims=True)
            den = (jnp.broadcast_to(den, (total, HD)) * any_chosen).reshape(2 * count, chunk, HD)
            dens = dens + jnp.sum(
                jnp.where(lane3 == row3 + k * chunk, den, 0.0), axis=1, keepdims=True
            )
            all_weights.append(jnp.concatenate([w0, w1], axis=-1).astype(jnp.bfloat16))
        den_send[:, span] = dens.reshape(NX, places[1] - places[0], 2, 1, HD)
        if opening:
            swap(1).wait_recv()
        for k in range(heads_here):
            values = kv[1, :, k].reshape(2 * rows, images * HD)
            pulled = jnp.dot(all_weights[k], values, preferred_element_type=jnp.float32)
            num = pulled[:, :HD] * chosen[0]
            for j in range(1, images):
                num = num + pulled[:, j * HD : (j + 1) * HD] * chosen[j]
            num_send[:, span, :, k] = num.astype(jnp.bfloat16).reshape(
                NX, places[1] - places[0], 2, chunk, HD
            )
        for dx in (2, 1, 3):
            start(
                return_pair(
                    (num_send.at[dx, span], den_send.at[dx, span]),
                    (num_x.at[dx, span], den_x.at[dx, span]),
                    index,
                    3 + index,
                    device(lax.rem(x - dx + NX, NX), zh, zl, core),
                )
            )

    def pass_return(places, index):
        span = slice(*places)
        settle_return(num_x.at[1:NX, span], den_x.at[1:NX, span], 3 + index)
        num = num_send[0, span].astype(jnp.float32)
        den = den_send[0, span]
        for dx in range(1, NX):
            num = num + num_x[dx, span].astype(jnp.float32)
            den = den + den_x[dx, span]
        num_pass[span] = num.astype(jnp.bfloat16)
        den_pass[span] = den
        for place in range(*places):
            for half in range(2 if place else 1):
                to_half = half if place else 1 - zl
                start(
                    return_pair(
                        (num_pass.at[place, to_half], den_pass.at[place, to_half]),
                        (num_z.at[place * 2 + zl], den_z.at[place * 2 + zl]),
                        6,
                        7,
                        device(x, lax.rem(zh - SHIFTS[place] + NZH, NZH), to_half, core),
                    )
                )

    one_to = slice(1, NX)
    settle_queries((0, slice(*AWAY)), 4)
    pass_queries(AWAY, 2, 7)
    settle_queries((0, slice(*NEAR)), 5)
    pass_queries(NEAR, 3, 8)
    settle_queries((one_to, slice(*OWN)), 6)
    attend(OWN, 0, True)
    settle_queries((one_to, slice(*AWAY)), 7)
    attend(AWAY, 1, False)
    settle_queries((one_to, slice(*NEAR)), 8)
    attend(NEAR, 2, False)
    pass_return(OWN, 0)
    num_z[zl] = num_pass[0, zl]
    den_z[zl] = den_pass[0, zl]
    pass_return(AWAY, 1)
    pass_return(NEAR, 2)

    settle_queries((0, one_to), 0)
    settle_queries((one_to, slice(*OWN)), 1)
    settle_queries((one_to, slice(*AWAY)), 2)
    settle_queries((one_to, slice(*NEAR)), 3)
    swap(0).wait_send()
    swap(1).wait_send()
    for index, places in enumerate((OWN, AWAY, NEAR)):
        span = slice(*places)
        settle_return(num_x.at[one_to, span], den_x.at[one_to, span], index)
    settle_return(num_z.at[1:NZ], den_z.at[1:NZ], 6)
    settle_return(num_z.at[1:NZ], den_z.at[1:NZ], 7)

    den_total = jnp.sum(den_z[...], axis=0)
    pair_rows = heads_here * chunk
    lane2 = lax.broadcasted_iota(jnp.int32, (pair_rows, HD), 1)
    row2 = lax.broadcasted_iota(jnp.int32, (pair_rows, HD), 0)
    den_column = jnp.sum(
        jnp.where(lane2 == row2, jnp.broadcast_to(den_total, (pair_rows, HD)), 0.0),
        axis=-1,
        keepdims=True,
    )
    num_total = jnp.sum(num_z[...].astype(jnp.float32), axis=0).reshape(pair_rows, HD)
    context = num_total / den_column
    for head in range(heads_here * group_size):
        out[:, head * HD : (head + 1) * HD] = context[head * 4 : (head + 1) * 4, :].astype(
            jnp.bfloat16
        )


def local(
    patch_store,
    w_key,
    w_value,
    key_gain,
    query_gain,
    queries,
    owner_table,
    reader_table,
    request_image,
    image_tiles,
):
    images, rows, width = patch_store.shape
    kv_width = w_key.shape[1]
    heads_here = kv_width // HD
    group_size = queries.shape[1] // kv_width
    steps = width // KC
    chunk = group_size * 4
    groups, reads = reader_table.shape
    vmem = pl.BlockSpec(memory_space=pltpu.VMEM)
    hbm = pl.BlockSpec(memory_space=pl.ANY)
    dma = pltpu.SemaphoreType.DMA
    return pl.pallas_call(
        kernel,
        out_shape=jax.ShapeDtypeStruct((4, queries.shape[1]), jnp.bfloat16),
        in_specs=[hbm] * 10,
        out_specs=vmem,
        scratch_shapes=[
            pltpu.VMEM((steps, images, rows, KC), jnp.bfloat16),
            pltpu.VMEM((width, kv_width), jnp.bfloat16),
            pltpu.VMEM((width, kv_width), jnp.bfloat16),
            pltpu.VMEM((images * rows, kv_width), jnp.float32),
            pltpu.VMEM((images * rows, kv_width), jnp.float32),
            pltpu.VMEM((2, 2, heads_here, rows, images * HD), jnp.bfloat16),
            pltpu.VMEM(queries.shape, jnp.bfloat16),
            pltpu.VMEM((1, HD), jnp.float32),
            pltpu.VMEM((1, HD), jnp.float32),
            pltpu.SMEM(owner_table.shape, jnp.int32),
            pltpu.SMEM((reads, groups), jnp.int32),
            pltpu.SMEM(request_image.shape, jnp.int32),
            pltpu.SMEM(image_tiles.shape, jnp.int32),
            pltpu.VMEM((heads_here * group_size, queries.shape[0], HD), jnp.float32),
            pltpu.VMEM((2, heads_here, chunk, HD), jnp.bfloat16),
            pltpu.VMEM((1, HD), jnp.float32),
            pltpu.VMEM((NX, NZH, 2, heads_here, chunk, HD), jnp.bfloat16),
            pltpu.VMEM((NX, NZH, 1, HD), jnp.float32),
            pltpu.VMEM((NX, NZH, 2, heads_here, chunk, HD), jnp.bfloat16),
            pltpu.VMEM((NX, NZH, 2, 1, HD), jnp.float32),
            pltpu.VMEM((NX, NZH, 2, heads_here, chunk, HD), jnp.bfloat16),
            pltpu.VMEM((NX, NZH, 2, 1, HD), jnp.float32),
            pltpu.VMEM((NZH, 2, heads_here, chunk, HD), jnp.bfloat16),
            pltpu.VMEM((NZH, 2, 1, HD), jnp.float32),
            pltpu.VMEM((NZ, heads_here, chunk, HD), jnp.bfloat16),
            pltpu.VMEM((NZ, 1, HD), jnp.float32),
            dma((7,)),
            dma((steps,)),
            dma((2, width // WC)),
            dma((4,)),
            dma((9,)),
            dma((9,)),
            dma((8,)),
            dma((8,)),
        ],
        compiler_params=pltpu.CompilerParams(
            collective_id=0, has_side_effects=True, vmem_limit_bytes=56 * 1024 * 1024
        ),
        name="attend",
    )(
        patch_store,
        w_key,
        w_value,
        key_gain[None],
        query_gain[None],
        queries,
        owner_table,
        reader_table.T,
        request_image,
        image_tiles,
    )


def solution(mesh):
    placed = (
        P("wide", "depth", None),
        P(None, "narrow"),
        P(None, "narrow"),
        P(),
        P(),
        P("wide", "narrow"),
        P(),
        P(),
        P("wide"),
        P(),
    )
    return jax.shard_map(
        local, mesh=mesh, in_specs=placed, out_specs=P(("wide", "depth"), "narrow"), check_vma=False
    )
```

```python
import math

import jax
import jax.numpy as jnp
from jax import lax
from jax.experimental import pallas as pl
from jax.experimental.pallas import tpu as pltpu
from jax.sharding import PartitionSpec as P

HD = 128
EPS = 1e-05
NX = 4
NZH = 4
NZ = 8
SHIFTS = (0, 1, 3, 2)
OWN, NEAR, AWAY = (0, 1), (1, 3), (3, 4)
KC = 512
FIRST = 256
AHEAD = 3
SEND_AFTER = 1
MESH = pl.DeviceIdType.MESH


def steps_of(width):
    edges = [0, FIRST, *range(2 * FIRST, width + 1, KC)]
    return [slice(a, b) for a, b in zip(edges, edges[1:])]


def kernel(
    patches,
    w_key,
    w_value,
    key_gain_in,
    query_gain_in,
    queries_in,
    owner_in,
    reader_in,
    request_in,
    tiles_in,
    out,
    pbuf,
    kbuf,
    vbuf,
    acc_k,
    acc_v,
    kv,
    queries,
    key_gain,
    query_gain,
    owner_table,
    reader_table,
    request_image,
    image_tiles,
    q_norm,
    q_own,
    code_own,
    q_all,
    code_all,
    num_send,
    den_send,
    num_x,
    den_x,
    num_pass,
    den_pass,
    num_z,
    den_z,
    small_sem,
    fetch_sem,
    kv_sem,
    q_sem,
    code_sem,
    num_sem,
    den_sem,
):
    images, rows, width = patches.shape
    spans = steps_of(width)
    kv_width = w_key.shape[1]
    heads_here = kv_width // HD
    group_size = queries.shape[1] // kv_width
    wide = lax.axis_index("wide")
    narrow = lax.axis_index("narrow")
    depth = lax.axis_index("depth")
    x, zh = lax.rem(wide, NX), lax.div(wide, NX)
    zl, core = lax.div(depth, 2), lax.rem(depth, 2)
    z = zh * 2 + zl

    def device(x_to, zh_to, zl_to, core_to):
        return (zh_to * NX + x_to, narrow, zl_to * 2 + core_to)

    partner = device(x, zh, zl, 1 - core)

    barrier = pltpu.get_barrier_semaphore()
    for dz in (4, 3, 5, 2, 6, 1, 7):
        z_to = lax.rem(z + dz, NZ)
        pl.semaphore_signal(
            barrier,
            inc=1,
            device_id=device(x, lax.div(z_to, 2), lax.rem(z_to, 2), core),
            device_id_type=MESH,
        )
    for dx in (2, 1, 3):
        pl.semaphore_signal(
            barrier,
            inc=1,
            device_id=device(lax.rem(x + dx, NX), zh, zl, core),
            device_id_type=MESH,
        )
    pl.semaphore_signal(barrier, inc=1, device_id=partner, device_id_type=MESH)

    small = [
        pltpu.make_async_copy(source, target, small_sem.at[i])
        for i, (source, target) in enumerate(
            (
                (queries_in, queries),
                (query_gain_in, query_gain),
                (request_in, request_image),
                (reader_in, reader_table),
                (owner_in, owner_table),
                (tiles_in, image_tiles),
                (key_gain_in, key_gain),
            )
        )
    ]
    for copy in small:
        copy.start()

    def fetch(step):
        span = spans[step]
        for source, target in (
            (patches.at[:, :, span], pbuf.at[:, :, span]),
            (w_key.at[span, :], kbuf.at[span, :]),
            (w_value.at[span, :], vbuf.at[span, :]),
        ):
            pltpu.make_async_copy(source, target, fetch_sem.at[step]).start()

    def settle(ref, sem):
        pltpu.make_async_copy(ref, ref, sem).wait()

    def fetched(step):
        columns = spans[step].stop - spans[step].start
        together = columns * (images * rows + 2 * kv_width) // kv_width
        settle(kbuf.at[0:together, :], fetch_sem.at[step])

    for step in range(AHEAD):
        fetch(step)

    small[0].wait()
    small[1].wait()
    mine = queries[...].astype(jnp.float32)
    gain = query_gain[...]
    for head in range(heads_here * group_size):
        part = mine[:, head * HD : (head + 1) * HD]
        mean = jnp.mean(part * part, axis=-1, keepdims=True)
        q_norm[head] = part * lax.rsqrt(mean + EPS) * gain
    for half in range(2):
        for k in range(heads_here):
            own_rows = [
                q_norm[k * group_size + g, pl.ds(8 * half + 4 * core, 4), :]
                for g in range(group_size)
            ]
            q_own[half, k] = jnp.concatenate(own_rows, axis=0).astype(jnp.bfloat16)
    lanes = lax.broadcasted_iota(jnp.int32, (1, HD), 1)
    codes = jnp.zeros((1, HD), jnp.float32)
    for copy in small[2:]:
        copy.wait()
    for half in range(2):
        for r in range(4):
            image = reader_table[request_image[8 * half + 4 * core + r], wide]
            code = owner_table[image] * 8 + image_tiles[image]
            codes = jnp.where(lanes == half * 4 + r, code.astype(jnp.float32), codes)
    code_own[...] = codes
    q_all[0, 0] = q_own[...]
    code_all[0, 0] = codes

    def pair(sources, targets, send, recv, to):
        return [
            pltpu.make_async_remote_copy(
                src_ref=source,
                dst_ref=target,
                send_sem=sems.at[send],
                recv_sem=sems.at[recv],
                device_id=to,
                device_id_type=MESH,
            )
            for source, target, sems in zip(sources, targets, (q_sem, code_sem))
        ]

    def start(copies):
        for copy in copies:
            copy.start()

    def send_queries():
        pl.semaphore_wait(barrier, NZ - 1 + NX - 1 + 1)
        for d in (3, 2, 1):
            z_to = lax.rem(z + NZ + (2 * zl - 1) * d, NZ)
            zh_to = lax.div(z_to, 2)
            dzh = lax.rem(zh_to - zh + NZH, NZH)
            place = jnp.where(dzh == 2, 3, jnp.where(dzh == 3, 2, dzh))
            start(
                pair(
                    (q_own, code_own),
                    (q_all.at[0, place], code_all.at[0, place]),
                    0,
                    4 if d == 3 else 5,
                    device(x, zh_to, lax.rem(z_to, 2), core),
                )
            )
        for dx in (2, 1, 3):
            start(
                pair(
                    (q_own, code_own),
                    (q_all.at[dx, 0], code_all.at[dx, 0]),
                    1,
                    6,
                    device(lax.rem(x + dx, NX), zh, zl, core),
                )
            )

    def pass_queries(places, send, recv):
        span = slice(*places)
        for dx in (2, 1, 3):
            start(
                pair(
                    (q_all.at[0, span], code_all.at[0, span]),
                    (q_all.at[dx, span], code_all.at[dx, span]),
                    send,
                    recv,
                    device(lax.rem(x + dx, NX), zh, zl, core),
                )
            )

    def settle_queries(where, index):
        settle(q_all.at[where], q_sem.at[index])
        settle(code_all.at[where], code_sem.at[index])

    def project(acc, block, weight, step):
        product = jnp.dot(block, weight[spans[step], :], preferred_element_type=jnp.float32)
        if step == 0:
            acc[...] = product
        else:
            acc[...] += product

    for step in range(len(spans)):
        if step + AHEAD < len(spans):
            fetch(step + AHEAD)
        fetched(step)
        block = pbuf[:, :, spans[step]].reshape(images * rows, -1)
        project(acc_k, block, kbuf, step)
        project(acc_v, block, vbuf, step)
        if step == SEND_AFTER:
            send_queries()

    def swap(which):
        return pltpu.make_async_remote_copy(
            src_ref=kv.at[which, core],
            dst_ref=kv.at[which, core],
            send_sem=kv_sem.at[which],
            recv_sem=kv_sem.at[2 + which],
            device_id=partner,
            device_id_type=MESH,
        )

    chunk = group_size * 4
    per_slot = 2 * chunk
    scale = 1.0 / math.sqrt(HD)
    first_slot = (wide * images * 8).astype(jnp.float32)
    tile = (zl * 2).astype(jnp.float32)

    def return_pair(sources, targets, send, recv, to):
        return [
            pltpu.make_async_remote_copy(
                src_ref=source,
                dst_ref=target,
                send_sem=sems.at[send],
                recv_sem=sems.at[recv],
                device_id=to,
                device_id_type=MESH,
            )
            for source, target, sems in zip(sources, targets, (num_sem, den_sem))
        ]

    def settle_return(num, den, index):
        settle(num, num_sem.at[index])
        settle(den, den_sem.at[index])

    def attend(places, index, opening):
        span = slice(*places)
        count = NX * (places[1] - places[0])
        total = count * per_slot
        lane = lax.broadcasted_iota(jnp.int32, (count, per_slot, HD), 2)
        row = lax.broadcasted_iota(jnp.int32, (count, per_slot, HD), 1)
        wanted = lax.div(row, chunk) * 4 + lax.rem(row, 4)
        spread = jnp.where(
            lane == wanted, jnp.broadcast_to(code_all[:, span].reshape(count, 1, HD), lane.shape), 0.0
        )
        column = jnp.sum(spread, axis=-1, keepdims=True).reshape(total, 1)
        local = jnp.broadcast_to(column, (total, HD)) - first_slot
        chosen, second = [], jnp.zeros((total, HD), jnp.float32)
        for j in range(images):
            below = local < 8.0 * j + 7.0
            chosen.append(jnp.where((local > 8.0 * j + tile) & below, 1.0, 0.0))
            second = jnp.where((local > 8.0 * j + tile + 1.0) & below, 1.0, second)
        any_chosen = chosen[0]
        for j in range(1, images):
            any_chosen = any_chosen + chosen[j]
        lane3 = lax.broadcasted_iota(jnp.int32, (2 * count, chunk, HD), 2)
        row3 = lax.broadcasted_iota(jnp.int32, (2 * count, chunk, HD), 1)
        dens = jnp.zeros((2 * count, 1, HD), jnp.float32)
        all_weights = []
        for k in range(heads_here):
            q = q_all[:, span, :, k].reshape(total, HD)
            expanded = jnp.concatenate(
                [q * chosen[j].astype(jnp.bfloat16) for j in range(images)], axis=-1
            )
            if opening and k == 0:
                swap(0).wait_recv()
            keys = kv[0, :, k].reshape(2 * rows, images * HD)
            scores = lax.dot_general(
                expanded, keys, (((1,), (1,)), ((), ())), preferred_element_type=jnp.float32
            )
            weights = jnp.exp(scores * scale)
            w0 = weights[:, :rows]
            w1 = weights[:, rows:] * jnp.concatenate([second] * (rows // HD), axis=-1)
            summed = w0 + w1
            folded = summed[:, :HD]
            for i in range(1, rows // HD):
                folded = folded + summed[:, i * HD : (i + 1) * HD]
            den = jnp.sum(folded, axis=-1, keepdims=True)
            den = (jnp.broadcast_to(den, (total, HD)) * any_chosen).reshape(2 * count, chunk, HD)
            dens = dens + jnp.sum(
                jnp.where(lane3 == row3 + k * chunk, den, 0.0), axis=1, keepdims=True
            )
            all_weights.append(jnp.concatenate([w0, w1], axis=-1).astype(jnp.bfloat16))
        den_send[:, span] = dens.reshape(NX, places[1] - places[0], 2, 1, HD)
        if opening:
            swap(1).wait_recv()
        for k in range(heads_here):
            values = kv[1, :, k].reshape(2 * rows, images * HD)
            pulled = jnp.dot(all_weights[k], values, preferred_element_type=jnp.float32)
            num = pulled[:, :HD] * chosen[0]
            for j in range(1, images):
                num = num + pulled[:, j * HD : (j + 1) * HD] * chosen[j]
            num_send[:, span, :, k] = num.astype(jnp.bfloat16).reshape(
                NX, places[1] - places[0], 2, chunk, HD
            )
        for dx in (2, 1, 3):
            start(
                return_pair(
                    (num_send.at[dx, span], den_send.at[dx, span]),
                    (num_x.at[dx, span], den_x.at[dx, span]),
                    index,
                    3 + index,
                    device(lax.rem(x - dx + NX, NX), zh, zl, core),
                )
            )

    def pass_return(places, index):
        span = slice(*places)
        settle_return(num_x.at[1:NX, span], den_x.at[1:NX, span], 3 + index)
        num = num_send[0, span].astype(jnp.float32)
        den = den_send[0, span]
        for dx in range(1, NX):
            num = num + num_x[dx, span].astype(jnp.float32)
            den = den + den_x[dx, span]
        num_pass[span] = num.astype(jnp.bfloat16)
        den_pass[span] = den
        for place in range(*places):
            for half in range(2 if place else 1):
                to_half = half if place else 1 - zl
                start(
                    return_pair(
                        (num_pass.at[place, to_half], den_pass.at[place, to_half]),
                        (num_z.at[place * 2 + zl], den_z.at[place * 2 + zl]),
                        6,
                        7,
                        device(x, lax.rem(zh - SHIFTS[place] + NZH, NZH), to_half, core),
                    )
                )

    one_to = slice(1, NX)
    settle_queries((0, slice(*AWAY)), 4)
    pass_queries(AWAY, 2, 7)
    settle_queries((0, slice(*NEAR)), 5)
    pass_queries(NEAR, 3, 8)

    gain = key_gain[...]
    for k in range(heads_here):
        for j in range(images):
            raw = acc_k[j * rows : (j + 1) * rows, k * HD : (k + 1) * HD]
            mean = jnp.mean(raw * raw, axis=-1, keepdims=True)
            kv[0, core, k, :, j * HD : (j + 1) * HD] = (
                raw * lax.rsqrt(mean + EPS) * gain
            ).astype(jnp.bfloat16)
    swap(0).start()
    for k in range(heads_here):
        for j in range(images):
            kv[1, core, k, :, j * HD : (j + 1) * HD] = acc_v[
                j * rows : (j + 1) * rows, k * HD : (k + 1) * HD
            ].astype(jnp.bfloat16)
    swap(1).start()

    settle_queries((one_to, slice(*OWN)), 6)
    attend(OWN, 0, True)
    settle_queries((one_to, slice(*AWAY)), 7)
    attend(AWAY, 1, False)
    settle_queries((one_to, slice(*NEAR)), 8)
    attend(NEAR, 2, False)
    pass_return(OWN, 0)
    num_z[zl] = num_pass[0, zl]
    den_z[zl] = den_pass[0, zl]
    pass_return(AWAY, 1)
    pass_return(NEAR, 2)

    settle_queries((0, one_to), 0)
    settle_queries((one_to, slice(*OWN)), 1)
    settle_queries((one_to, slice(*AWAY)), 2)
    settle_queries((one_to, slice(*NEAR)), 3)
    swap(0).wait_send()
    swap(1).wait_send()
    for index, places in enumerate((OWN, AWAY, NEAR)):
        span = slice(*places)
        settle_return(num_x.at[one_to, span], den_x.at[one_to, span], index)
    settle_return(num_z.at[1:NZ], den_z.at[1:NZ], 6)
    settle_return(num_z.at[1:NZ], den_z.at[1:NZ], 7)

    den_total = jnp.sum(den_z[...], axis=0)
    pair_rows = heads_here * chunk
    lane2 = lax.broadcasted_iota(jnp.int32, (pair_rows, HD), 1)
    row2 = lax.broadcasted_iota(jnp.int32, (pair_rows, HD), 0)
    den_column = jnp.sum(
        jnp.where(lane2 == row2, jnp.broadcast_to(den_total, (pair_rows, HD)), 0.0),
        axis=-1,
        keepdims=True,
    )
    num_total = jnp.sum(num_z[...].astype(jnp.float32), axis=0).reshape(pair_rows, HD)
    context = num_total / den_column
    for head in range(heads_here * group_size):
        out[:, head * HD : (head + 1) * HD] = context[head * 4 : (head + 1) * 4, :].astype(
            jnp.bfloat16
        )


def local(
    patch_store,
    w_key,
    w_value,
    key_gain,
    query_gain,
    queries,
    owner_table,
    reader_table,
    request_image,
    image_tiles,
):
    images, rows, width = patch_store.shape
    kv_width = w_key.shape[1]
    heads_here = kv_width // HD
    group_size = queries.shape[1] // kv_width
    chunk = group_size * 4
    groups, reads = reader_table.shape
    vmem = pl.BlockSpec(memory_space=pltpu.VMEM)
    hbm = pl.BlockSpec(memory_space=pl.ANY)
    dma = pltpu.SemaphoreType.DMA
    return pl.pallas_call(
        kernel,
        out_shape=pltpu.VMEM((4, queries.shape[1]), jnp.bfloat16),
        in_specs=[hbm] * 10,
        out_specs=vmem,
        scratch_shapes=[
            pltpu.VMEM(patch_store.shape, jnp.bfloat16),
            pltpu.VMEM((width, kv_width), jnp.bfloat16),
            pltpu.VMEM((width, kv_width), jnp.bfloat16),
            pltpu.VMEM((images * rows, kv_width), jnp.float32),
            pltpu.VMEM((images * rows, kv_width), jnp.float32),
            pltpu.VMEM((2, 2, heads_here, rows, images * HD), jnp.bfloat16),
            pltpu.VMEM(queries.shape, jnp.bfloat16),
            pltpu.VMEM((1, HD), jnp.float32),
            pltpu.VMEM((1, HD), jnp.float32),
            pltpu.SMEM(owner_table.shape, jnp.int32),
            pltpu.SMEM((reads, groups), jnp.int32),
            pltpu.SMEM(request_image.shape, jnp.int32),
            pltpu.SMEM(image_tiles.shape, jnp.int32),
            pltpu.VMEM((heads_here * group_size, queries.shape[0], HD), jnp.float32),
            pltpu.VMEM((2, heads_here, chunk, HD), jnp.bfloat16),
            pltpu.VMEM((1, HD), jnp.float32),
            pltpu.VMEM((NX, NZH, 2, heads_here, chunk, HD), jnp.bfloat16),
            pltpu.VMEM((NX, NZH, 1, HD), jnp.float32),
            pltpu.VMEM((NX, NZH, 2, heads_here, chunk, HD), jnp.bfloat16),
            pltpu.VMEM((NX, NZH, 2, 1, HD), jnp.float32),
            pltpu.VMEM((NX, NZH, 2, heads_here, chunk, HD), jnp.bfloat16),
            pltpu.VMEM((NX, NZH, 2, 1, HD), jnp.float32),
            pltpu.VMEM((NZH, 2, heads_here, chunk, HD), jnp.bfloat16),
            pltpu.VMEM((NZH, 2, 1, HD), jnp.float32),
            pltpu.VMEM((NZ, heads_here, chunk, HD), jnp.bfloat16),
            pltpu.VMEM((NZ, 1, HD), jnp.float32),
            dma((7,)),
            dma((len(steps_of(width)),)),
            dma((4,)),
            dma((9,)),
            dma((9,)),
            dma((8,)),
            dma((8,)),
        ],
        compiler_params=pltpu.CompilerParams(
            collective_id=0, has_side_effects=True, vmem_limit_bytes=56 * 1024 * 1024
        ),
        name="attend",
    )(
        patch_store,
        w_key,
        w_value,
        key_gain[None],
        query_gain[None],
        queries,
        owner_table,
        reader_table.T,
        request_image,
        image_tiles,
    )


def solution(mesh):
    placed = (
        P("wide", "depth", None),
        P(None, "narrow"),
        P(None, "narrow"),
        P(),
        P(),
        P("wide", "narrow"),
        P(),
        P(),
        P("wide"),
        P(),
    )
    return jax.shard_map(
        local, mesh=mesh, in_specs=placed, out_specs=P(("wide", "depth"), "narrow"), check_vma=False
    )
```

```python
import math

import jax
import jax.numpy as jnp
from jax import lax
from jax.experimental import pallas as pl
from jax.experimental.pallas import tpu as pltpu
from jax.sharding import PartitionSpec as P

HD = 128
EPS = 1e-05
NX = 4
NZH = 4
NZ = 8
SHIFTS = (0, 1, 3, 2)
OWN, NEAR, AWAY = (0, 1), (1, 3), (3, 4)
KC = 512
FIRST = 256
AHEAD = 3
SEND_AFTER = 1
MESH = pl.DeviceIdType.MESH


def steps_of(width):
    edges = [0, FIRST, *range(2 * FIRST, width + 1, KC)]
    return [slice(a, b) for a, b in zip(edges, edges[1:])]


def kernel(
    patches,
    w_key,
    w_value,
    key_gain_in,
    query_gain_in,
    queries_in,
    owner_in,
    reader_in,
    request_in,
    tiles_in,
    out,
    pbuf,
    kbuf,
    vbuf,
    acc_k,
    acc_v,
    kv,
    queries,
    key_gain,
    query_gain,
    owner_table,
    reader_table,
    request_image,
    image_tiles,
    q_norm,
    q_own,
    code_own,
    q_all,
    code_all,
    num_send,
    den_send,
    num_x,
    den_x,
    num_pass,
    den_pass,
    num_z,
    den_z,
    tally,
    small_sem,
    fetch_sem,
    kv_sem,
    q_sem,
    num_sem,
):
    images, rows, width = patches.shape
    spans = steps_of(width)
    kv_width = w_key.shape[1]
    heads_here = kv_width // HD
    group_size = queries.shape[1] // kv_width
    wide = lax.axis_index("wide")
    narrow = lax.axis_index("narrow")
    depth = lax.axis_index("depth")
    x, zh = lax.rem(wide, NX), lax.div(wide, NX)
    zl, core = lax.div(depth, 2), lax.rem(depth, 2)
    z = zh * 2 + zl

    def device(x_to, zh_to, zl_to, core_to):
        return (zh_to * NX + x_to, narrow, zl_to * 2 + core_to)

    partner = device(x, zh, zl, 1 - core)

    barrier = pltpu.get_barrier_semaphore()
    for dz in (3, 5, 2, 6, 1, 7):
        z_to = lax.rem(z + dz, NZ)
        pl.semaphore_signal(
            barrier,
            inc=1,
            device_id=device(x, lax.div(z_to, 2), lax.rem(z_to, 2), core),
            device_id_type=MESH,
        )
    for dx in (2, 1, 3):
        pl.semaphore_signal(
            barrier,
            inc=1,
            device_id=device(lax.rem(x + dx, NX), zh, zl, core),
            device_id_type=MESH,
        )
    pl.semaphore_signal(barrier, inc=1, device_id=partner, device_id_type=MESH)

    small = [
        pltpu.make_async_copy(source, target, small_sem.at[i])
        for i, (source, target) in enumerate(
            (
                (queries_in, queries),
                (query_gain_in, query_gain),
                (request_in, request_image),
                (reader_in, reader_table),
                (owner_in, owner_table),
                (tiles_in, image_tiles),
                (key_gain_in, key_gain),
            )
        )
    ]
    for copy in small:
        copy.start()

    def fetch(step):
        span = spans[step]
        for source, target in (
            (patches.at[:, :, span], pbuf.at[:, :, span]),
            (w_key.at[span, :], kbuf.at[span, :]),
            (w_value.at[span, :], vbuf.at[span, :]),
        ):
            pltpu.make_async_copy(source, target, fetch_sem.at[step]).start()

    def settle(ref, sem):
        pltpu.make_async_copy(ref, ref, sem).wait()

    def fetched(step):
        columns = spans[step].stop - spans[step].start
        together = columns * (images * rows + 2 * kv_width) // kv_width
        settle(kbuf.at[0:together, :], fetch_sem.at[step])

    for step in range(AHEAD):
        fetch(step)

    small[0].wait()
    small[1].wait()
    mine = queries[...].astype(jnp.float32)
    gain = query_gain[...]
    for head in range(heads_here * group_size):
        part = mine[:, head * HD : (head + 1) * HD]
        mean = jnp.mean(part * part, axis=-1, keepdims=True)
        q_norm[head] = part * lax.rsqrt(mean + EPS) * gain
    for half in range(2):
        for k in range(heads_here):
            own_rows = [
                q_norm[k * group_size + g, pl.ds(8 * half + 4 * core, 4), :]
                for g in range(group_size)
            ]
            q_own[half, k] = jnp.concatenate(own_rows, axis=0).astype(jnp.bfloat16)
    lanes = lax.broadcasted_iota(jnp.int32, (1, HD), 1)
    codes = jnp.zeros((1, HD), jnp.float32)
    for copy in small[2:]:
        copy.wait()
    for half in range(2):
        for r in range(4):
            image = reader_table[request_image[8 * half + 4 * core + r], wide]
            code = owner_table[image] * 8 + image_tiles[image]
            codes = jnp.where(lanes == half * 4 + r, code.astype(jnp.float32), codes)
    code_own[...] = codes
    q_all[0, 0] = q_own[...]
    code_all[0, 0] = codes

    def pair(sources, targets, recv, to):
        return [
            pltpu.make_async_remote_copy(
                src_ref=source,
                dst_ref=target,
                send_sem=q_sem.at[0],
                recv_sem=q_sem.at[recv],
                device_id=to,
                device_id_type=MESH,
            )
            for source, target in zip(sources, targets)
        ]

    def start(copies):
        for copy in copies:
            copy.start()

    def send_queries():
        pl.semaphore_wait(barrier, NZ - 2 + NX - 1 + 1)
        for d in (3, 2, 1):
            z_to = lax.rem(z + NZ + (2 * zl - 1) * d, NZ)
            zh_to = lax.div(z_to, 2)
            dzh = lax.rem(zh_to - zh + NZH, NZH)
            place = jnp.where(dzh == 2, 3, jnp.where(dzh == 3, 2, dzh))
            start(
                pair(
                    (q_own, code_own),
                    (q_all.at[0, place], code_all.at[0, place]),
                    1 if d == 3 else 2,
                    device(x, zh_to, lax.rem(z_to, 2), core),
                )
            )
        for dx in (2, 1, 3):
            start(
                pair(
                    (q_own, code_own),
                    (q_all.at[dx, 0], code_all.at[dx, 0]),
                    3,
                    device(lax.rem(x + dx, NX), zh, zl, core),
                )
            )

    def pass_queries(places, recv):
        span = slice(*places)
        for dx in (2, 1, 3):
            start(
                pair(
                    (q_all.at[0, span], code_all.at[0, span]),
                    (q_all.at[dx, span], code_all.at[dx, span]),
                    recv,
                    device(lax.rem(x + dx, NX), zh, zl, core),
                )
            )

    slot_rows = 2 * heads_here * group_size * 4 // 2 + 1
    chunk_rows = heads_here * group_size * 4 // 2 + 1

    def settle_queries(slots, index):
        settle(tally.at[0 : slots * slot_rows], q_sem.at[index])

    def settle_return(chunks, index):
        settle(tally.at[0 : chunks * chunk_rows], num_sem.at[index])

    def project(acc, block, weight, step):
        product = jnp.dot(block, weight[spans[step], :], preferred_element_type=jnp.float32)
        if step == 0:
            acc[...] = product
        else:
            acc[...] += product

    for step in range(len(spans)):
        if step + AHEAD < len(spans):
            fetch(step + AHEAD)
        fetched(step)
        block = pbuf[:, :, spans[step]].reshape(images * rows, -1)
        project(acc_k, block, kbuf, step)
        project(acc_v, block, vbuf, step)
        if step == SEND_AFTER:
            send_queries()

    def swap(which):
        return pltpu.make_async_remote_copy(
            src_ref=kv.at[which, core],
            dst_ref=kv.at[which, core],
            send_sem=kv_sem.at[which],
            recv_sem=kv_sem.at[2 + which],
            device_id=partner,
            device_id_type=MESH,
        )

    chunk = group_size * 4
    per_slot = 2 * chunk
    scale = 1.0 / math.sqrt(HD)
    first_slot = (wide * images * 8).astype(jnp.float32)
    tile = (zl * 2).astype(jnp.float32)

    def return_pair(sources, targets, recv, to):
        return [
            pltpu.make_async_remote_copy(
                src_ref=source,
                dst_ref=target,
                send_sem=num_sem.at[0],
                recv_sem=num_sem.at[recv],
                device_id=to,
                device_id_type=MESH,
            )
            for source, target in zip(sources, targets)
        ]

    def attend(places, index, opening):
        span = slice(*places)
        count = NX * (places[1] - places[0])
        total = count * per_slot
        lane = lax.broadcasted_iota(jnp.int32, (count, per_slot, HD), 2)
        row = lax.broadcasted_iota(jnp.int32, (count, per_slot, HD), 1)
        wanted = lax.div(row, chunk) * 4 + lax.rem(row, 4)
        spread = jnp.where(
            lane == wanted, jnp.broadcast_to(code_all[:, span].reshape(count, 1, HD), lane.shape), 0.0
        )
        column = jnp.sum(spread, axis=-1, keepdims=True).reshape(total, 1)
        local = jnp.broadcast_to(column, (total, HD)) - first_slot
        chosen, second = [], jnp.zeros((total, HD), jnp.float32)
        for j in range(images):
            below = local < 8.0 * j + 7.0
            chosen.append(jnp.where((local > 8.0 * j + tile) & below, 1.0, 0.0))
            second = jnp.where((local > 8.0 * j + tile + 1.0) & below, 1.0, second)
        any_chosen = chosen[0]
        for j in range(1, images):
            any_chosen = any_chosen + chosen[j]
        lane3 = lax.broadcasted_iota(jnp.int32, (2 * count, chunk, HD), 2)
        row3 = lax.broadcasted_iota(jnp.int32, (2 * count, chunk, HD), 1)
        dens = jnp.zeros((2 * count, 1, HD), jnp.float32)
        all_weights = []
        for k in range(heads_here):
            q = q_all[:, span, :, k].reshape(total, HD)
            expanded = jnp.concatenate(
                [q * chosen[j].astype(jnp.bfloat16) for j in range(images)], axis=-1
            )
            if opening and k == 0:
                swap(0).wait_recv()
            keys = kv[0, :, k].reshape(2 * rows, images * HD)
            scores = lax.dot_general(
                expanded, keys, (((1,), (1,)), ((), ())), preferred_element_type=jnp.float32
            )
            weights = jnp.exp(scores * scale)
            w0 = weights[:, :rows]
            w1 = weights[:, rows:] * jnp.concatenate([second] * (rows // HD), axis=-1)
            summed = w0 + w1
            folded = summed[:, :HD]
            for i in range(1, rows // HD):
                folded = folded + summed[:, i * HD : (i + 1) * HD]
            den = jnp.sum(folded, axis=-1, keepdims=True)
            den = (jnp.broadcast_to(den, (total, HD)) * any_chosen).reshape(2 * count, chunk, HD)
            dens = dens + jnp.sum(
                jnp.where(lane3 == row3 + k * chunk, den, 0.0), axis=1, keepdims=True
            )
            all_weights.append(jnp.concatenate([w0, w1], axis=-1).astype(jnp.bfloat16))
        den_send[:, span] = dens.reshape(NX, places[1] - places[0], 2, 1, HD)
        if opening:
            swap(1).wait_recv()
        for k in range(heads_here):
            values = kv[1, :, k].reshape(2 * rows, images * HD)
            pulled = jnp.dot(all_weights[k], values, preferred_element_type=jnp.float32)
            num = pulled[:, :HD] * chosen[0]
            for j in range(1, images):
                num = num + pulled[:, j * HD : (j + 1) * HD] * chosen[j]
            num_send[:, span, :, k] = num.astype(jnp.bfloat16).reshape(
                NX, places[1] - places[0], 2, chunk, HD
            )
        for dx in (2, 1, 3):
            start(
                return_pair(
                    (num_send.at[dx, span], den_send.at[dx, span]),
                    (num_x.at[dx, span], den_x.at[dx, span]),
                    1 + index,
                    device(lax.rem(x - dx + NX, NX), zh, zl, core),
                )
            )

    def pass_return(places, index):
        span = slice(*places)
        settle_return((NX - 1) * 2 * (places[1] - places[0]), 1 + index)
        num = num_send[0, span].astype(jnp.float32)
        den = den_send[0, span]
        for dx in range(1, NX):
            num = num + num_x[dx, span].astype(jnp.float32)
            den = den + den_x[dx, span]
        num_pass[span] = num.astype(jnp.bfloat16)
        den_pass[span] = den
        for place in range(*places):
            for half in range(2 if place else 1):
                to_half = half if place else 1 - zl
                start(
                    return_pair(
                        (num_pass.at[place, to_half], den_pass.at[place, to_half]),
                        (num_z.at[place * 2 + zl], den_z.at[place * 2 + zl]),
                        4,
                        device(x, lax.rem(zh - SHIFTS[place] + NZH, NZH), to_half, core),
                    )
                )

    settle_queries(1, 1)
    pass_queries(AWAY, 4)
    settle_queries(2, 2)
    pass_queries(NEAR, 5)

    gain = key_gain[...]
    for k in range(heads_here):
        for j in range(images):
            raw = acc_k[j * rows : (j + 1) * rows, k * HD : (k + 1) * HD]
            mean = jnp.mean(raw * raw, axis=-1, keepdims=True)
            kv[0, core, k, :, j * HD : (j + 1) * HD] = (
                raw * lax.rsqrt(mean + EPS) * gain
            ).astype(jnp.bfloat16)
    swap(0).start()
    for k in range(heads_here):
        for j in range(images):
            kv[1, core, k, :, j * HD : (j + 1) * HD] = acc_v[
                j * rows : (j + 1) * rows, k * HD : (k + 1) * HD
            ].astype(jnp.bfloat16)
    swap(1).start()

    settle_queries(NX - 1, 3)
    attend(OWN, 0, True)
    settle_queries(NX - 1, 4)
    attend(AWAY, 1, False)
    settle_queries(2 * (NX - 1), 5)
    attend(NEAR, 2, False)
    pass_return(OWN, 0)
    num_z[zl] = num_pass[0, zl]
    den_z[zl] = den_pass[0, zl]
    pass_return(AWAY, 1)
    pass_return(NEAR, 2)

    settle_queries(NX * NZH - 1, 0)
    swap(0).wait_send()
    swap(1).wait_send()
    settle_return((NX - 1) * NZ + NZ - 1, 0)
    settle_return(NZ - 1, 4)

    den_total = jnp.sum(den_z[...], axis=0)
    pair_rows = heads_here * chunk
    lane2 = lax.broadcasted_iota(jnp.int32, (pair_rows, HD), 1)
    row2 = lax.broadcasted_iota(jnp.int32, (pair_rows, HD), 0)
    den_column = jnp.sum(
        jnp.where(lane2 == row2, jnp.broadcast_to(den_total, (pair_rows, HD)), 0.0),
        axis=-1,
        keepdims=True,
    )
    num_total = jnp.sum(num_z[...].astype(jnp.float32), axis=0).reshape(pair_rows, HD)
    context = num_total / den_column
    for head in range(heads_here * group_size):
        out[:, head * HD : (head + 1) * HD] = context[head * 4 : (head + 1) * 4, :].astype(
            jnp.bfloat16
        )


def local(
    patch_store,
    w_key,
    w_value,
    key_gain,
    query_gain,
    queries,
    owner_table,
    reader_table,
    request_image,
    image_tiles,
):
    images, rows, width = patch_store.shape
    kv_width = w_key.shape[1]
    heads_here = kv_width // HD
    group_size = queries.shape[1] // kv_width
    chunk = group_size * 4
    groups, reads = reader_table.shape
    vmem = pl.BlockSpec(memory_space=pltpu.VMEM)
    hbm = pl.BlockSpec(memory_space=pl.ANY)
    dma = pltpu.SemaphoreType.DMA
    return pl.pallas_call(
        kernel,
        out_shape=pltpu.VMEM((4, queries.shape[1]), jnp.bfloat16),
        in_specs=[hbm] * 10,
        out_specs=vmem,
        scratch_shapes=[
            pltpu.VMEM(patch_store.shape, jnp.bfloat16),
            pltpu.VMEM((width, kv_width), jnp.bfloat16),
            pltpu.VMEM((width, kv_width), jnp.bfloat16),
            pltpu.VMEM((images * rows, kv_width), jnp.float32),
            pltpu.VMEM((images * rows, kv_width), jnp.float32),
            pltpu.VMEM((2, 2, heads_here, rows, images * HD), jnp.bfloat16),
            pltpu.VMEM(queries.shape, jnp.bfloat16),
            pltpu.VMEM((1, HD), jnp.float32),
            pltpu.VMEM((1, HD), jnp.float32),
            pltpu.SMEM(owner_table.shape, jnp.int32),
            pltpu.SMEM((reads, groups), jnp.int32),
            pltpu.SMEM(request_image.shape, jnp.int32),
            pltpu.SMEM(image_tiles.shape, jnp.int32),
            pltpu.VMEM((heads_here * group_size, queries.shape[0], HD), jnp.float32),
            pltpu.VMEM((2, heads_here, chunk, HD), jnp.bfloat16),
            pltpu.VMEM((1, HD), jnp.float32),
            pltpu.VMEM((NX, NZH, 2, heads_here, chunk, HD), jnp.bfloat16),
            pltpu.VMEM((NX, NZH, 1, HD), jnp.float32),
            pltpu.VMEM((NX, NZH, 2, heads_here, chunk, HD), jnp.bfloat16),
            pltpu.VMEM((NX, NZH, 2, 1, HD), jnp.float32),
            pltpu.VMEM((NX, NZH, 2, heads_here, chunk, HD), jnp.bfloat16),
            pltpu.VMEM((NX, NZH, 2, 1, HD), jnp.float32),
            pltpu.VMEM((NZH, 2, heads_here, chunk, HD), jnp.bfloat16),
            pltpu.VMEM((NZH, 2, 1, HD), jnp.float32),
            pltpu.VMEM((NZ, heads_here, chunk, HD), jnp.bfloat16),
            pltpu.VMEM((NZ, 1, HD), jnp.float32),
            pltpu.VMEM(((NX * NZ - 1) * (heads_here * chunk // 2 + 1), 1, HD), jnp.float32),
            dma((7,)),
            dma((len(steps_of(width)),)),
            dma((4,)),
            dma((6,)),
            dma((5,)),
        ],
        compiler_params=pltpu.CompilerParams(
            collective_id=0, has_side_effects=True, vmem_limit_bytes=56 * 1024 * 1024
        ),
        name="attend",
    )(
        patch_store,
        w_key,
        w_value,
        key_gain[None],
        query_gain[None],
        queries,
        owner_table,
        reader_table.T,
        request_image,
        image_tiles,
    )


def solution(mesh):
    placed = (
        P("wide", "depth", None),
        P(None, "narrow"),
        P(None, "narrow"),
        P(),
        P(),
        P("wide", "narrow"),
        P(),
        P(),
        P("wide"),
        P(),
    )
    return jax.shard_map(
        local, mesh=mesh, in_specs=placed, out_specs=P(("wide", "depth"), "narrow"), check_vma=False
    )
```

```python
import math

import jax
import jax.numpy as jnp
from jax import lax
from jax.experimental import pallas as pl
from jax.experimental.pallas import tpu as pltpu
from jax.sharding import PartitionSpec as P

HD = 128
EPS = 1e-05
NX = 4
NZH = 4
NZ = 8
SHIFTS = (0, 1, 3, 2)
OWN, NEAR, AWAY = (0, 1), (1, 3), (3, 4)
KC = 512
FIRST = 256
AHEAD = 3
SEND_AFTER = 1
MESH = pl.DeviceIdType.MESH


def steps_of(width):
    edges = [0, FIRST, *range(2 * FIRST, width + 1, KC)]
    return [slice(a, b) for a, b in zip(edges, edges[1:])]


def kernel(
    patches,
    w_key,
    w_value,
    key_gain_in,
    query_gain_in,
    queries_in,
    owner_in,
    reader_in,
    request_in,
    tiles_in,
    out,
    pbuf,
    kbuf,
    vbuf,
    acc_k,
    acc_v,
    kv,
    queries,
    key_gain,
    query_gain,
    owner_table,
    reader_table,
    request_image,
    image_tiles,
    q_norm,
    q_own,
    code_own,
    q_all,
    code_all,
    num_send,
    den_send,
    num_x,
    den_x,
    num_pass,
    den_pass,
    num_z,
    den_z,
    tally,
    small_sem,
    fetch_sem,
    kv_sem,
    q_sem,
    num_sem,
):
    images, rows, width = patches.shape
    spans = steps_of(width)
    kv_width = w_key.shape[1]
    heads_here = kv_width // HD
    group_size = queries.shape[1] // kv_width
    wide = lax.axis_index("wide")
    narrow = lax.axis_index("narrow")
    depth = lax.axis_index("depth")
    x, zh = lax.rem(wide, NX), lax.div(wide, NX)
    zl, core = lax.div(depth, 2), lax.rem(depth, 2)
    z = zh * 2 + zl

    def device(x_to, zh_to, zl_to, core_to):
        return (zh_to * NX + x_to, narrow, zl_to * 2 + core_to)

    partner = device(x, zh, zl, 1 - core)

    barrier = pltpu.get_barrier_semaphore()
    for dz in (3, 5, 2, 6, 1, 7):
        z_to = lax.rem(z + dz, NZ)
        pl.semaphore_signal(
            barrier,
            inc=1,
            device_id=device(x, lax.div(z_to, 2), lax.rem(z_to, 2), core),
            device_id_type=MESH,
        )
    for dx in (2, 1, 3):
        pl.semaphore_signal(
            barrier,
            inc=1,
            device_id=device(lax.rem(x + dx, NX), zh, zl, core),
            device_id_type=MESH,
        )
    pl.semaphore_signal(barrier, inc=1, device_id=partner, device_id_type=MESH)

    small = [
        pltpu.make_async_copy(source, target, small_sem.at[i])
        for i, (source, target) in enumerate(
            (
                (queries_in, queries),
                (query_gain_in, query_gain),
                (request_in, request_image),
                (reader_in, reader_table),
                (owner_in, owner_table),
                (tiles_in, image_tiles),
                (key_gain_in, key_gain),
            )
        )
    ]
    for copy in small:
        copy.start()

    def fetch(step):
        span = spans[step]
        for source, target in (
            (patches.at[:, :, span], pbuf.at[:, :, span]),
            (w_key.at[span, :], kbuf.at[span, :]),
            (w_value.at[span, :], vbuf.at[span, :]),
        ):
            pltpu.make_async_copy(source, target, fetch_sem.at[step]).start()

    def settle(ref, sem):
        pltpu.make_async_copy(ref, ref, sem).wait()

    def fetched(step):
        columns = spans[step].stop - spans[step].start
        together = columns * (images * rows + 2 * kv_width) // kv_width
        settle(kbuf.at[0:together, :], fetch_sem.at[step])

    for step in range(AHEAD):
        fetch(step)

    small[0].wait()
    small[1].wait()
    mine = queries[...].astype(jnp.float32)
    gain = query_gain[...]
    for head in range(heads_here * group_size):
        part = mine[:, head * HD : (head + 1) * HD]
        mean = jnp.mean(part * part, axis=-1, keepdims=True)
        q_norm[head] = part * lax.rsqrt(mean + EPS) * gain
    for half in range(2):
        for k in range(heads_here):
            own_rows = [
                q_norm[k * group_size + g, pl.ds(8 * half + 4 * core, 4), :]
                for g in range(group_size)
            ]
            q_own[half, k] = jnp.concatenate(own_rows, axis=0).astype(jnp.bfloat16)
    lanes = lax.broadcasted_iota(jnp.int32, (1, HD), 1)
    codes = jnp.zeros((1, HD), jnp.float32)
    for copy in small[2:]:
        copy.wait()
    for half in range(2):
        for r in range(4):
            image = reader_table[request_image[8 * half + 4 * core + r], wide]
            code = owner_table[image] * 8 + image_tiles[image]
            codes = jnp.where(lanes == half * 4 + r, code.astype(jnp.float32), codes)
    code_own[...] = codes
    q_all[0, 0] = q_own[...]
    code_all[0, 0] = codes

    def pair(sources, targets, recv, to):
        return [
            pltpu.make_async_remote_copy(
                src_ref=source,
                dst_ref=target,
                send_sem=q_sem.at[0],
                recv_sem=q_sem.at[recv],
                device_id=to,
                device_id_type=MESH,
            )
            for source, target in zip(sources, targets)
        ]

    def start(copies):
        for copy in copies:
            copy.start()

    def send_queries():
        pl.semaphore_wait(barrier, NZ - 2 + NX - 1 + 1)
        for d in (3, 2, 1):
            z_to = lax.rem(z + NZ + (2 * zl - 1) * d, NZ)
            zh_to = lax.div(z_to, 2)
            dzh = lax.rem(zh_to - zh + NZH, NZH)
            place = jnp.where(dzh == 2, 3, jnp.where(dzh == 3, 2, dzh))
            start(
                pair(
                    (q_own, code_own),
                    (q_all.at[0, place], code_all.at[0, place]),
                    1 if d == 3 else 2,
                    device(x, zh_to, lax.rem(z_to, 2), core),
                )
            )
        for dx in (2, 1, 3):
            start(
                pair(
                    (q_own, code_own),
                    (q_all.at[dx, 0], code_all.at[dx, 0]),
                    3,
                    device(lax.rem(x + dx, NX), zh, zl, core),
                )
            )

    def pass_queries(places, recv):
        span = slice(*places)
        for dx in (2, 1, 3):
            start(
                pair(
                    (q_all.at[0, span], code_all.at[0, span]),
                    (q_all.at[dx, span], code_all.at[dx, span]),
                    recv,
                    device(lax.rem(x + dx, NX), zh, zl, core),
                )
            )

    slot_rows = 2 * heads_here * group_size * 4 // 2 + 1
    chunk_rows = heads_here * group_size * 4 // 2 + 1

    def settle_queries(slots, index):
        settle(tally.at[0 : slots * slot_rows], q_sem.at[index])

    def settle_return(chunks, index):
        settle(tally.at[0 : chunks * chunk_rows], num_sem.at[index])

    def project(acc, block, weight, step):
        product = jnp.dot(block, weight[spans[step], :], preferred_element_type=jnp.float32)
        if step == 0:
            acc[...] = product
        else:
            acc[...] += product

    for step in range(len(spans)):
        if step + AHEAD < len(spans):
            fetch(step + AHEAD)
        fetched(step)
        block = pbuf[:, :, spans[step]].reshape(images * rows, -1)
        project(acc_k, block, kbuf, step)
        project(acc_v, block, vbuf, step)
        if step == SEND_AFTER:
            send_queries()

    def swap(which):
        return pltpu.make_async_remote_copy(
            src_ref=kv.at[which, core],
            dst_ref=kv.at[which, core],
            send_sem=kv_sem.at[which],
            recv_sem=kv_sem.at[2 + which],
            device_id=partner,
            device_id_type=MESH,
        )

    chunk = group_size * 4
    per_slot = 2 * chunk
    scale = 1.0 / (math.sqrt(HD) * math.log(2.0))
    first_slot = (wide * images * 8).astype(jnp.float32)
    tile = (zl * 2).astype(jnp.float32)

    def return_pair(sources, targets, recv, to):
        return [
            pltpu.make_async_remote_copy(
                src_ref=source,
                dst_ref=target,
                send_sem=num_sem.at[0],
                recv_sem=num_sem.at[recv],
                device_id=to,
                device_id_type=MESH,
            )
            for source, target in zip(sources, targets)
        ]

    def attend(places, index, opening):
        span = slice(*places)
        count = NX * (places[1] - places[0])
        total = count * per_slot
        lane = lax.broadcasted_iota(jnp.int32, (count, per_slot, HD), 2)
        row = lax.broadcasted_iota(jnp.int32, (count, per_slot, HD), 1)
        wanted = lax.div(row, chunk) * 4 + lax.rem(row, 4)
        spread = jnp.where(
            lane == wanted, jnp.broadcast_to(code_all[:, span].reshape(count, 1, HD), lane.shape), 0.0
        )
        column = jnp.sum(spread, axis=-1, keepdims=True).reshape(total, 1)
        local = jnp.broadcast_to(column, (total, HD)) - first_slot
        chosen, second = [], jnp.zeros((total, HD), jnp.float32)
        for j in range(images):
            below = local < 8.0 * j + 7.0
            chosen.append(jnp.where((local > 8.0 * j + tile) & below, 1.0, 0.0))
            second = jnp.where((local > 8.0 * j + tile + 1.0) & below, 1.0, second)
        any_chosen = chosen[0]
        for j in range(1, images):
            any_chosen = any_chosen + chosen[j]
        lane3 = lax.broadcasted_iota(jnp.int32, (2 * count, chunk, HD), 2)
        row3 = lax.broadcasted_iota(jnp.int32, (2 * count, chunk, HD), 1)
        dens = jnp.zeros((2 * count, 1, HD), jnp.float32)
        all_weights = []
        for k in range(heads_here):
            q = q_all[:, span, :, k].reshape(total, HD)
            expanded = jnp.concatenate(
                [q * chosen[j].astype(jnp.bfloat16) for j in range(images)], axis=-1
            )
            if opening and k == 0:
                swap(0).wait_recv()
            keys = kv[0, :, k].reshape(2 * rows, images * HD)
            scores = lax.dot_general(
                expanded, keys, (((1,), (1,)), ((), ())), preferred_element_type=jnp.float32
            )
            weights = jnp.exp2(scores * scale)
            w0 = weights[:, :rows]
            w1 = weights[:, rows:] * jnp.concatenate([second] * (rows // HD), axis=-1)
            summed = w0 + w1
            folded = summed[:, :HD]
            for i in range(1, rows // HD):
                folded = folded + summed[:, i * HD : (i + 1) * HD]
            den = jnp.sum(folded, axis=-1, keepdims=True)
            den = (jnp.broadcast_to(den, (total, HD)) * any_chosen).reshape(2 * count, chunk, HD)
            dens = dens + jnp.sum(
                jnp.where(lane3 == row3 + k * chunk, den, 0.0), axis=1, keepdims=True
            )
            all_weights.append(jnp.concatenate([w0, w1], axis=-1).astype(jnp.bfloat16))
        den_send[:, span] = dens.reshape(NX, places[1] - places[0], 2, 1, HD)
        if opening:
            swap(1).wait_recv()
        for k in range(heads_here):
            values = kv[1, :, k].reshape(2 * rows, images * HD)
            pulled = jnp.dot(all_weights[k], values, preferred_element_type=jnp.float32)
            num = pulled[:, :HD] * chosen[0]
            for j in range(1, images):
                num = num + pulled[:, j * HD : (j + 1) * HD] * chosen[j]
            num_send[:, span, :, k] = num.astype(jnp.bfloat16).reshape(
                NX, places[1] - places[0], 2, chunk, HD
            )
        for dx in (2, 1, 3):
            start(
                return_pair(
                    (num_send.at[dx, span], den_send.at[dx, span]),
                    (num_x.at[dx, span], den_x.at[dx, span]),
                    1 + index,
                    device(lax.rem(x - dx + NX, NX), zh, zl, core),
                )
            )

    def pass_return(places, index):
        span = slice(*places)
        settle_return((NX - 1) * 2 * (places[1] - places[0]), 1 + index)
        num = num_send[0, span].astype(jnp.float32)
        den = den_send[0, span]
        for dx in range(1, NX):
            num = num + num_x[dx, span].astype(jnp.float32)
            den = den + den_x[dx, span]
        num_pass[span] = num.astype(jnp.bfloat16)
        den_pass[span] = den
        for place in range(*places):
            for half in range(2 if place else 1):
                to_half = half if place else 1 - zl
                start(
                    return_pair(
                        (num_pass.at[place, to_half], den_pass.at[place, to_half]),
                        (num_z.at[place * 2 + zl], den_z.at[place * 2 + zl]),
                        4,
                        device(x, lax.rem(zh - SHIFTS[place] + NZH, NZH), to_half, core),
                    )
                )

    settle_queries(1, 1)
    pass_queries(AWAY, 4)
    settle_queries(2, 2)
    pass_queries(NEAR, 5)

    gain = key_gain[...]
    for k in range(heads_here):
        for j in range(images):
            raw = acc_k[j * rows : (j + 1) * rows, k * HD : (k + 1) * HD]
            mean = jnp.mean(raw * raw, axis=-1, keepdims=True)
            kv[0, core, k, :, j * HD : (j + 1) * HD] = (
                raw * lax.rsqrt(mean + EPS) * gain
            ).astype(jnp.bfloat16)
    swap(0).start()
    for k in range(heads_here):
        for j in range(images):
            kv[1, core, k, :, j * HD : (j + 1) * HD] = acc_v[
                j * rows : (j + 1) * rows, k * HD : (k + 1) * HD
            ].astype(jnp.bfloat16)
    swap(1).start()

    settle_queries(NX - 1, 3)
    attend(OWN, 0, True)
    settle_queries(NX - 1, 4)
    attend(AWAY, 1, False)
    settle_queries(2 * (NX - 1), 5)
    attend(NEAR, 2, False)
    pass_return(OWN, 0)
    num_z[zl] = num_pass[0, zl]
    den_z[zl] = den_pass[0, zl]
    pass_return(AWAY, 1)
    pass_return(NEAR, 2)

    settle_queries(NX * NZH - 1, 0)
    swap(0).wait_send()
    swap(1).wait_send()
    settle_return((NX - 1) * NZ + NZ - 1, 0)
    settle_return(NZ - 1, 4)

    den_total = jnp.sum(den_z[...], axis=0)
    pair_rows = heads_here * chunk
    lane2 = lax.broadcasted_iota(jnp.int32, (pair_rows, HD), 1)
    row2 = lax.broadcasted_iota(jnp.int32, (pair_rows, HD), 0)
    den_column = jnp.sum(
        jnp.where(lane2 == row2, jnp.broadcast_to(den_total, (pair_rows, HD)), 0.0),
        axis=-1,
        keepdims=True,
    )
    num_total = jnp.sum(num_z[...].astype(jnp.float32), axis=0).reshape(pair_rows, HD)
    context = num_total / den_column
    for head in range(heads_here * group_size):
        out[:, head * HD : (head + 1) * HD] = context[head * 4 : (head + 1) * 4, :].astype(
            jnp.bfloat16
        )


def local(
    patch_store,
    w_key,
    w_value,
    key_gain,
    query_gain,
    queries,
    owner_table,
    reader_table,
    request_image,
    image_tiles,
):
    images, rows, width = patch_store.shape
    kv_width = w_key.shape[1]
    heads_here = kv_width // HD
    group_size = queries.shape[1] // kv_width
    chunk = group_size * 4
    groups, reads = reader_table.shape
    vmem = pl.BlockSpec(memory_space=pltpu.VMEM)
    hbm = pl.BlockSpec(memory_space=pl.ANY)
    dma = pltpu.SemaphoreType.DMA
    return pl.pallas_call(
        kernel,
        out_shape=pltpu.VMEM((4, queries.shape[1]), jnp.bfloat16),
        in_specs=[hbm] * 10,
        out_specs=vmem,
        scratch_shapes=[
            pltpu.VMEM(patch_store.shape, jnp.bfloat16),
            pltpu.VMEM((width, kv_width), jnp.bfloat16),
            pltpu.VMEM((width, kv_width), jnp.bfloat16),
            pltpu.VMEM((images * rows, kv_width), jnp.float32),
            pltpu.VMEM((images * rows, kv_width), jnp.float32),
            pltpu.VMEM((2, 2, heads_here, rows, images * HD), jnp.bfloat16),
            pltpu.VMEM(queries.shape, jnp.bfloat16),
            pltpu.VMEM((1, HD), jnp.float32),
            pltpu.VMEM((1, HD), jnp.float32),
            pltpu.SMEM(owner_table.shape, jnp.int32),
            pltpu.SMEM((reads, groups), jnp.int32),
            pltpu.SMEM(request_image.shape, jnp.int32),
            pltpu.SMEM(image_tiles.shape, jnp.int32),
            pltpu.VMEM((heads_here * group_size, queries.shape[0], HD), jnp.float32),
            pltpu.VMEM((2, heads_here, chunk, HD), jnp.bfloat16),
            pltpu.VMEM((1, HD), jnp.float32),
            pltpu.VMEM((NX, NZH, 2, heads_here, chunk, HD), jnp.bfloat16),
            pltpu.VMEM((NX, NZH, 1, HD), jnp.float32),
            pltpu.VMEM((NX, NZH, 2, heads_here, chunk, HD), jnp.bfloat16),
            pltpu.VMEM((NX, NZH, 2, 1, HD), jnp.float32),
            pltpu.VMEM((NX, NZH, 2, heads_here, chunk, HD), jnp.bfloat16),
            pltpu.VMEM((NX, NZH, 2, 1, HD), jnp.float32),
            pltpu.VMEM((NZH, 2, heads_here, chunk, HD), jnp.bfloat16),
            pltpu.VMEM((NZH, 2, 1, HD), jnp.float32),
            pltpu.VMEM((NZ, heads_here, chunk, HD), jnp.bfloat16),
            pltpu.VMEM((NZ, 1, HD), jnp.float32),
            pltpu.VMEM(((NX * NZ - 1) * (heads_here * chunk // 2 + 1), 1, HD), jnp.float32),
            dma((7,)),
            dma((len(steps_of(width)),)),
            dma((4,)),
            dma((6,)),
            dma((5,)),
        ],
        compiler_params=pltpu.CompilerParams(
            collective_id=0, has_side_effects=True, vmem_limit_bytes=56 * 1024 * 1024
        ),
        name="attend",
    )(
        patch_store,
        w_key,
        w_value,
        key_gain[None],
        query_gain[None],
        queries,
        owner_table,
        reader_table.T,
        request_image,
        image_tiles,
    )


def solution(mesh):
    placed = (
        P("wide", "depth", None),
        P(None, "narrow"),
        P(None, "narrow"),
        P(),
        P(),
        P("wide", "narrow"),
        P(),
        P(),
        P("wide"),
        P(),
    )
    return jax.shard_map(
        local, mesh=mesh, in_specs=placed, out_specs=P(("wide", "depth"), "narrow"), check_vma=False
    )
```

```python
import math

import jax
import jax.numpy as jnp
from jax import lax
from jax.experimental import pallas as pl
from jax.experimental.pallas import tpu as pltpu
from jax.sharding import PartitionSpec as P

HD = 128
EPS = 1e-05
NX = 4
NZH = 4
NZ = 8
SHIFTS = (0, 1, 3, 2)
OWN, NEAR, AWAY = (0, 1), (1, 3), (3, 4)
KC = 512
FIRST = 256
AHEAD = 3
SEND_AFTER = 1
MESH = pl.DeviceIdType.MESH


def steps_of(width):
    edges = [0, FIRST, *range(2 * FIRST, width + 1, KC)]
    return [slice(a, b) for a, b in zip(edges, edges[1:])]


def kernel(
    patches,
    w_key,
    w_value,
    key_gain_in,
    query_gain_in,
    queries_in,
    owner_in,
    reader_in,
    request_in,
    tiles_in,
    out,
    pbuf,
    kbuf,
    vbuf,
    acc_k,
    acc_v,
    kv,
    queries,
    key_gain,
    query_gain,
    owner_table,
    reader_table,
    request_image,
    image_tiles,
    q_norm,
    q_own,
    code_own,
    q_all,
    code_all,
    num_send,
    den_send,
    num_x,
    den_x,
    num_pass,
    den_pass,
    num_z,
    den_z,
    tally,
    small_sem,
    fetch_sem,
    kv_sem,
    q_sem,
    num_sem,
):
    images, rows, width = patches.shape
    spans = steps_of(width)
    kv_width = w_key.shape[1]
    heads_here = kv_width // HD
    group_size = queries.shape[1] // kv_width
    wide = lax.axis_index("wide")
    narrow = lax.axis_index("narrow")
    depth = lax.axis_index("depth")
    x, zh = lax.rem(wide, NX), lax.div(wide, NX)
    zl, core = lax.div(depth, 2), lax.rem(depth, 2)
    z = zh * 2 + zl

    def device(x_to, zh_to, zl_to, core_to):
        return (zh_to * NX + x_to, narrow, zl_to * 2 + core_to)

    partner = device(x, zh, zl, 1 - core)

    barrier = pltpu.get_barrier_semaphore()
    for dz in (3, 5, 2, 6, 1, 7):
        z_to = lax.rem(z + dz, NZ)
        pl.semaphore_signal(
            barrier,
            inc=1,
            device_id=device(x, lax.div(z_to, 2), lax.rem(z_to, 2), core),
            device_id_type=MESH,
        )
    for dx in (2, 1, 3):
        pl.semaphore_signal(
            barrier,
            inc=1,
            device_id=device(lax.rem(x + dx, NX), zh, zl, core),
            device_id_type=MESH,
        )
    pl.semaphore_signal(barrier, inc=1, device_id=partner, device_id_type=MESH)

    small = [
        pltpu.make_async_copy(source, target, small_sem.at[i])
        for i, (source, target) in enumerate(
            (
                (queries_in, queries),
                (query_gain_in, query_gain),
                (request_in, request_image),
                (reader_in, reader_table),
                (owner_in, owner_table),
                (tiles_in, image_tiles),
                (key_gain_in, key_gain),
            )
        )
    ]
    for copy in small:
        copy.start()

    def fetch(step):
        span = spans[step]
        for source, target in (
            (patches.at[:, :, span], pbuf.at[:, :, span]),
            (w_key.at[span, :], kbuf.at[span, :]),
            (w_value.at[span, :], vbuf.at[span, :]),
        ):
            pltpu.make_async_copy(source, target, fetch_sem.at[step]).start()

    def settle(ref, sem):
        pltpu.make_async_copy(ref, ref, sem).wait()

    def fetched(step):
        columns = spans[step].stop - spans[step].start
        together = columns * (images * rows + 2 * kv_width) // kv_width
        settle(kbuf.at[0:together, :], fetch_sem.at[step])

    for step in range(AHEAD):
        fetch(step)

    small[0].wait()
    small[1].wait()
    mine = queries[...].astype(jnp.float32)
    gain = query_gain[...]
    for head in range(heads_here * group_size):
        part = mine[:, head * HD : (head + 1) * HD]
        mean = jnp.mean(part * part, axis=-1, keepdims=True)
        q_norm[head] = part * lax.rsqrt(mean + EPS) * gain
    for half in range(2):
        for k in range(heads_here):
            own_rows = [
                q_norm[k * group_size + g, pl.ds(8 * half + 4 * core, 4), :]
                for g in range(group_size)
            ]
            q_own[half, k] = jnp.concatenate(own_rows, axis=0).astype(jnp.bfloat16)
    lanes = lax.broadcasted_iota(jnp.int32, (1, HD), 1)
    codes = jnp.zeros((1, HD), jnp.float32)
    for copy in small[2:]:
        copy.wait()
    for half in range(2):
        for r in range(4):
            image = reader_table[request_image[8 * half + 4 * core + r], wide]
            code = owner_table[image] * 8 + image_tiles[image]
            codes = jnp.where(lanes == half * 4 + r, code.astype(jnp.float32), codes)
    code_own[...] = codes
    q_all[0, 0] = q_own[...]
    code_all[0, 0] = codes

    def pair(sources, targets, recv, to):
        return [
            pltpu.make_async_remote_copy(
                src_ref=source,
                dst_ref=target,
                send_sem=q_sem.at[0],
                recv_sem=q_sem.at[recv],
                device_id=to,
                device_id_type=MESH,
            )
            for source, target in zip(sources, targets)
        ]

    def start(copies):
        for copy in copies:
            copy.start()

    def send_queries():
        pl.semaphore_wait(barrier, NZ - 2 + NX - 1 + 1)
        for d in (3, 2, 1):
            z_to = lax.rem(z + NZ + (2 * zl - 1) * d, NZ)
            zh_to = lax.div(z_to, 2)
            dzh = lax.rem(zh_to - zh + NZH, NZH)
            place = jnp.where(dzh == 2, 3, jnp.where(dzh == 3, 2, dzh))
            start(
                pair(
                    (q_own, code_own),
                    (q_all.at[0, place], code_all.at[0, place]),
                    1 if d == 3 else 2,
                    device(x, zh_to, lax.rem(z_to, 2), core),
                )
            )
        for dx in (2, 1, 3):
            start(
                pair(
                    (q_own, code_own),
                    (q_all.at[dx, 0], code_all.at[dx, 0]),
                    3,
                    device(lax.rem(x + dx, NX), zh, zl, core),
                )
            )

    def pass_queries(places, recv):
        span = slice(*places)
        for dx in (2, 1, 3):
            start(
                pair(
                    (q_all.at[0, span], code_all.at[0, span]),
                    (q_all.at[dx, span], code_all.at[dx, span]),
                    recv,
                    device(lax.rem(x + dx, NX), zh, zl, core),
                )
            )

    slot_rows = 2 * heads_here * group_size * 4 // 2 + 1
    chunk_rows = heads_here * group_size * 4 // 2 + 1

    def settle_queries(slots, index):
        settle(tally.at[0 : slots * slot_rows], q_sem.at[index])

    def settle_return(chunks, index):
        settle(tally.at[0 : chunks * chunk_rows], num_sem.at[index])

    def project(acc, block, weight, step):
        product = jnp.dot(block, weight[spans[step], :], preferred_element_type=jnp.float32)
        if step == 0:
            acc[...] = product
        else:
            acc[...] += product

    for step in range(len(spans)):
        if step + AHEAD < len(spans):
            fetch(step + AHEAD)
        fetched(step)
        block = pbuf[:, :, spans[step]].reshape(images * rows, -1)
        project(acc_k, block, kbuf, step)
        project(acc_v, block, vbuf, step)
        if step == SEND_AFTER:
            send_queries()

    def swap(which, k):
        return pltpu.make_async_remote_copy(
            src_ref=kv.at[which, core, k],
            dst_ref=kv.at[which, core, k],
            send_sem=kv_sem.at[0, which, k],
            recv_sem=kv_sem.at[1, which, k],
            device_id=partner,
            device_id_type=MESH,
        )

    chunk = group_size * 4
    per_slot = 2 * chunk
    scale = 1.0 / math.sqrt(HD)
    first_slot = (wide * images * 8).astype(jnp.float32)
    tile = (zl * 2).astype(jnp.float32)

    def return_pair(sources, targets, recv, to):
        return [
            pltpu.make_async_remote_copy(
                src_ref=source,
                dst_ref=target,
                send_sem=num_sem.at[0],
                recv_sem=num_sem.at[recv],
                device_id=to,
                device_id_type=MESH,
            )
            for source, target in zip(sources, targets)
        ]

    def attend(places, index, opening):
        span = slice(*places)
        count = NX * (places[1] - places[0])
        total = count * per_slot
        lane = lax.broadcasted_iota(jnp.int32, (count, per_slot, HD), 2)
        row = lax.broadcasted_iota(jnp.int32, (count, per_slot, HD), 1)
        wanted = lax.div(row, chunk) * 4 + lax.rem(row, 4)
        spread = jnp.where(
            lane == wanted, jnp.broadcast_to(code_all[:, span].reshape(count, 1, HD), lane.shape), 0.0
        )
        column = jnp.sum(spread, axis=-1, keepdims=True).reshape(total, 1)
        local = jnp.broadcast_to(column, (total, HD)) - first_slot
        chosen, second = [], jnp.zeros((total, HD), jnp.float32)
        for j in range(images):
            below = local < 8.0 * j + 7.0
            chosen.append(jnp.where((local > 8.0 * j + tile) & below, 1.0, 0.0))
            second = jnp.where((local > 8.0 * j + tile + 1.0) & below, 1.0, second)
        any_chosen = chosen[0]
        for j in range(1, images):
            any_chosen = any_chosen + chosen[j]
        lane3 = lax.broadcasted_iota(jnp.int32, (2 * count, chunk, HD), 2)
        row3 = lax.broadcasted_iota(jnp.int32, (2 * count, chunk, HD), 1)
        dens = jnp.zeros((2 * count, 1, HD), jnp.float32)
        all_weights = []
        for k in range(heads_here):
            q = q_all[:, span, :, k].reshape(total, HD)
            expanded = jnp.concatenate(
                [q * chosen[j].astype(jnp.bfloat16) for j in range(images)], axis=-1
            )
            if opening:
                swap(0, k).wait_recv()
            keys = kv[0, :, k].reshape(2 * rows, images * HD)
            scores = lax.dot_general(
                expanded, keys, (((1,), (1,)), ((), ())), preferred_element_type=jnp.float32
            )
            weights = jnp.exp(scores * scale)
            w0 = weights[:, :rows]
            w1 = weights[:, rows:] * jnp.concatenate([second] * (rows // HD), axis=-1)
            summed = w0 + w1
            folded = summed[:, :HD]
            for i in range(1, rows // HD):
                folded = folded + summed[:, i * HD : (i + 1) * HD]
            den = jnp.sum(folded, axis=-1, keepdims=True)
            den = (jnp.broadcast_to(den, (total, HD)) * any_chosen).reshape(2 * count, chunk, HD)
            dens = dens + jnp.sum(
                jnp.where(lane3 == row3 + k * chunk, den, 0.0), axis=1, keepdims=True
            )
            all_weights.append(jnp.concatenate([w0, w1], axis=-1).astype(jnp.bfloat16))
        den_send[:, span] = dens.reshape(NX, places[1] - places[0], 2, 1, HD)
        for k in range(heads_here):
            if opening:
                swap(1, k).wait_recv()
            values = kv[1, :, k].reshape(2 * rows, images * HD)
            pulled = jnp.dot(all_weights[k], values, preferred_element_type=jnp.float32)
            num = pulled[:, :HD] * chosen[0]
            for j in range(1, images):
                num = num + pulled[:, j * HD : (j + 1) * HD] * chosen[j]
            num_send[:, span, :, k] = num.astype(jnp.bfloat16).reshape(
                NX, places[1] - places[0], 2, chunk, HD
            )
        for dx in (2, 1, 3):
            start(
                return_pair(
                    (num_send.at[dx, span], den_send.at[dx, span]),
                    (num_x.at[dx, span], den_x.at[dx, span]),
                    1 + index,
                    device(lax.rem(x - dx + NX, NX), zh, zl, core),
                )
            )

    def pass_return(places, index):
        span = slice(*places)
        settle_return((NX - 1) * 2 * (places[1] - places[0]), 1 + index)
        num = num_send[0, span].astype(jnp.float32)
        den = den_send[0, span]
        for dx in range(1, NX):
            num = num + num_x[dx, span].astype(jnp.float32)
            den = den + den_x[dx, span]
        num_pass[span] = num.astype(jnp.bfloat16)
        den_pass[span] = den
        for place in range(*places):
            for half in range(2 if place else 1):
                to_half = half if place else 1 - zl
                start(
                    return_pair(
                        (num_pass.at[place, to_half], den_pass.at[place, to_half]),
                        (num_z.at[place * 2 + zl], den_z.at[place * 2 + zl]),
                        4,
                        device(x, lax.rem(zh - SHIFTS[place] + NZH, NZH), to_half, core),
                    )
                )

    settle_queries(1, 1)
    pass_queries(AWAY, 4)
    settle_queries(2, 2)
    pass_queries(NEAR, 5)

    gain = key_gain[...]
    for k in range(heads_here):
        for j in range(images):
            raw = acc_k[j * rows : (j + 1) * rows, k * HD : (k + 1) * HD]
            mean = jnp.mean(raw * raw, axis=-1, keepdims=True)
            kv[0, core, k, :, j * HD : (j + 1) * HD] = (
                raw * lax.rsqrt(mean + EPS) * gain
            ).astype(jnp.bfloat16)
        swap(0, k).start()
    for k in range(heads_here):
        for j in range(images):
            kv[1, core, k, :, j * HD : (j + 1) * HD] = acc_v[
                j * rows : (j + 1) * rows, k * HD : (k + 1) * HD
            ].astype(jnp.bfloat16)
        swap(1, k).start()

    settle_queries(NX - 1, 3)
    attend(OWN, 0, True)
    settle_queries(NX - 1, 4)
    attend(AWAY, 1, False)
    settle_queries(2 * (NX - 1), 5)
    attend(NEAR, 2, False)
    pass_return(OWN, 0)
    num_z[zl] = num_pass[0, zl]
    den_z[zl] = den_pass[0, zl]
    pass_return(AWAY, 1)
    pass_return(NEAR, 2)

    settle_queries(NX * NZH - 1, 0)
    for k in range(heads_here):
        swap(0, k).wait_send()
        swap(1, k).wait_send()
    settle_return((NX - 1) * NZ + NZ - 1, 0)
    settle_return(NZ - 1, 4)

    den_total = jnp.sum(den_z[...], axis=0)
    pair_rows = heads_here * chunk
    lane2 = lax.broadcasted_iota(jnp.int32, (pair_rows, HD), 1)
    row2 = lax.broadcasted_iota(jnp.int32, (pair_rows, HD), 0)
    den_column = jnp.sum(
        jnp.where(lane2 == row2, jnp.broadcast_to(den_total, (pair_rows, HD)), 0.0),
        axis=-1,
        keepdims=True,
    )
    num_total = jnp.sum(num_z[...].astype(jnp.float32), axis=0).reshape(pair_rows, HD)
    context = num_total / den_column
    for head in range(heads_here * group_size):
        out[:, head * HD : (head + 1) * HD] = context[head * 4 : (head + 1) * 4, :].astype(
            jnp.bfloat16
        )


def local(
    patch_store,
    w_key,
    w_value,
    key_gain,
    query_gain,
    queries,
    owner_table,
    reader_table,
    request_image,
    image_tiles,
):
    images, rows, width = patch_store.shape
    kv_width = w_key.shape[1]
    heads_here = kv_width // HD
    group_size = queries.shape[1] // kv_width
    chunk = group_size * 4
    groups, reads = reader_table.shape
    vmem = pl.BlockSpec(memory_space=pltpu.VMEM)
    hbm = pl.BlockSpec(memory_space=pl.ANY)
    dma = pltpu.SemaphoreType.DMA
    return pl.pallas_call(
        kernel,
        out_shape=pltpu.VMEM((4, queries.shape[1]), jnp.bfloat16),
        in_specs=[hbm] * 10,
        out_specs=vmem,
        scratch_shapes=[
            pltpu.VMEM(patch_store.shape, jnp.bfloat16),
            pltpu.VMEM((width, kv_width), jnp.bfloat16),
            pltpu.VMEM((width, kv_width), jnp.bfloat16),
            pltpu.VMEM((images * rows, kv_width), jnp.float32),
            pltpu.VMEM((images * rows, kv_width), jnp.float32),
            pltpu.VMEM((2, 2, heads_here, rows, images * HD), jnp.bfloat16),
            pltpu.VMEM(queries.shape, jnp.bfloat16),
            pltpu.VMEM((1, HD), jnp.float32),
            pltpu.VMEM((1, HD), jnp.float32),
            pltpu.SMEM(owner_table.shape, jnp.int32),
            pltpu.SMEM((reads, groups), jnp.int32),
            pltpu.SMEM(request_image.shape, jnp.int32),
            pltpu.SMEM(image_tiles.shape, jnp.int32),
            pltpu.VMEM((heads_here * group_size, queries.shape[0], HD), jnp.float32),
            pltpu.VMEM((2, heads_here, chunk, HD), jnp.bfloat16),
            pltpu.VMEM((1, HD), jnp.float32),
            pltpu.VMEM((NX, NZH, 2, heads_here, chunk, HD), jnp.bfloat16),
            pltpu.VMEM((NX, NZH, 1, HD), jnp.float32),
            pltpu.VMEM((NX, NZH, 2, heads_here, chunk, HD), jnp.bfloat16),
            pltpu.VMEM((NX, NZH, 2, 1, HD), jnp.float32),
            pltpu.VMEM((NX, NZH, 2, heads_here, chunk, HD), jnp.bfloat16),
            pltpu.VMEM((NX, NZH, 2, 1, HD), jnp.float32),
            pltpu.VMEM((NZH, 2, heads_here, chunk, HD), jnp.bfloat16),
            pltpu.VMEM((NZH, 2, 1, HD), jnp.float32),
            pltpu.VMEM((NZ, heads_here, chunk, HD), jnp.bfloat16),
            pltpu.VMEM((NZ, 1, HD), jnp.float32),
            pltpu.VMEM(((NX * NZ - 1) * (heads_here * chunk // 2 + 1), 1, HD), jnp.float32),
            dma((7,)),
            dma((len(steps_of(width)),)),
            dma((2, 2, heads_here)),
            dma((6,)),
            dma((5,)),
        ],
        compiler_params=pltpu.CompilerParams(
            collective_id=0, has_side_effects=True, vmem_limit_bytes=56 * 1024 * 1024
        ),
        name="attend",
    )(
        patch_store,
        w_key,
        w_value,
        key_gain[None],
        query_gain[None],
        queries,
        owner_table,
        reader_table.T,
        request_image,
        image_tiles,
    )


def solution(mesh):
    placed = (
        P("wide", "depth", None),
        P(None, "narrow"),
        P(None, "narrow"),
        P(),
        P(),
        P("wide", "narrow"),
        P(),
        P(),
        P("wide"),
        P(),
    )
    return jax.shard_map(
        local, mesh=mesh, in_specs=placed, out_specs=P(("wide", "depth"), "narrow"), check_vma=False
    )
```
